32 devices in a mesh: dp: 4 (over z), fsdp: 8 (over y, x, core).
Axes of the slice: x: 2, y: 2, z: 4, core: 2. Of those that a mesh axis runs over, the one named last changes fastest.
Arguments:
- emb_grad: float32 [4, 8, 2048, 4608], P('dp', 'fsdp')
- mat_grad: float32 [4, 8, 128, 4608], P('dp', 'fsdp')
- norm_grad: float32 [4, 8, 9, 4608], P('dp', 'fsdp')
- emb_param: float32 [2048, 4608], P('fsdp')
- emb_mom: float32 [2048, 4608], P('fsdp')
- emb_var: float32 [2048, 4608], P('fsdp')
- mat_param: float32 [128, 4608], P('fsdp')
- mat_mom: float32 [128, 4608], P('fsdp')
- mat_var: float32 [128, 4608], P('fsdp')
- norm_param: float32 [9, 4608], P(None, 'fsdp')
- norm_mom: float32 [9, 4608], P(None, 'fsdp')
- norm_var: float32 [9, 4608], P(None, 'fsdp')
Outputs:
- output 1: float32 [2048, 4608], P('fsdp')
- output 2: float32 [2048, 4608], P('fsdp')
- output 3: float32 [2048, 4608], P('fsdp')
- output 4: bfloat16 [2048, 4608], P('fsdp')
- output 5: float32 [128, 4608], P('fsdp')
- output 6: float32 [128, 4608], P('fsdp')
- output 7: float32 [128, 4608], P('fsdp')
- output 8: bfloat16 [128, 4608], P('fsdp')
- output 9: float32 [9, 4608], P(None, 'fsdp')
- output 10: float32 [9, 4608], P(None, 'fsdp')
- output 11: float32 [9, 4608], P(None, 'fsdp')
- output 12: bfloat16 [9, 4608], P(None, 'fsdp')
All inputs are finite; a program needn't handle non-finite values.
Results may differ from the reference program's by a relative error of at most 0.001.
Values sent between devices are 32-bit elements.
A program may use at most 1 GiB of HBM per device.

```python
import math
import jax
import jax.numpy as jnp

DP_SIZE = 4
FSDP_SIZE = 8
WIDTH = 4608
EMB_ROWS = 256
MAT_ROWS = 16
NORM_COUNT = 9
ADAM_STEP = 10

LEARN_RATE = 0.003
BETA_ONE = 0.9
BETA_TWO = 0.95
ADAM_EPS = 1e-8
WEIGHT_DECAY = 0.1
CLIP_NORM = 1.0

DEV_COUNT = DP_SIZE * FSDP_SIZE
VOCAB_ROWS = FSDP_SIZE * EMB_ROWS
MATRIX_ROWS = FSDP_SIZE * MAT_ROWS
TOTAL_PARAMS = (VOCAB_ROWS + MATRIX_ROWS + NORM_COUNT) * WIDTH


def setup_inputs(seed: int = 0) -> dict:
    key_list = jax.random.split(jax.random.key(seed), 12)
    grad_unit = 2.0 / math.sqrt(TOTAL_PARAMS)
    spread = math.sqrt(DEV_COUNT)
    mom_unit = 0.5 * grad_unit
    row_frac = jnp.arange(VOCAB_ROWS, dtype=jnp.float32) / VOCAB_ROWS
    emb_scale = (2.0 / jnp.sqrt(1.0 + 15.0 * row_frac))[:, None]
    weight_scale = WIDTH ** -0.5
    emb_shape = (VOCAB_ROWS, WIDTH)
    mat_shape = (MATRIX_ROWS, WIDTH)
    norm_shape = (NORM_COUNT, WIDTH)
    dev_lead = (DP_SIZE, FSDP_SIZE)
    return {
        "emb_grad": spread * grad_unit * emb_scale * jax.random.normal(key_list[0], dev_lead + emb_shape, jnp.float32),
        "mat_grad": spread * grad_unit * jax.random.normal(key_list[1], dev_lead + mat_shape, jnp.float32),
        "norm_grad": spread * grad_unit * jax.random.normal(key_list[2], dev_lead + norm_shape, jnp.float32),
        "emb_param": weight_scale * jax.random.normal(key_list[3], emb_shape, jnp.float32),
        "emb_mom": 0.1 * mom_unit * emb_scale * jax.random.normal(key_list[4], emb_shape, jnp.float32),
        "emb_var": 0.05 * (mom_unit * emb_scale) ** 2 * jax.random.uniform(key_list[5], emb_shape, jnp.float32, 0.5, 1.5),
        "mat_param": weight_scale * jax.random.normal(key_list[6], mat_shape, jnp.float32),
        "mat_mom": 0.1 * mom_unit * jax.random.normal(key_list[7], mat_shape, jnp.float32),
        "mat_var": 0.05 * mom_unit ** 2 * jax.random.uniform(key_list[8], mat_shape, jnp.float32, 0.5, 1.5),
        "norm_param": 0.1 * jax.random.normal(key_list[9], norm_shape, jnp.float32),
        "norm_mom": 0.1 * mom_unit * jax.random.normal(key_list[10], norm_shape, jnp.float32),
        "norm_var": 0.05 * mom_unit ** 2 * jax.random.uniform(key_list[11], norm_shape, jnp.float32, 0.5, 1.5),
    }


def adamw_update(grad_part, param_old, mom_old, var_old, decay_rate):
    new_mom = BETA_ONE * mom_old + (1.0 - BETA_ONE) * grad_part
    new_var = BETA_TWO * var_old + (1.0 - BETA_TWO) * grad_part * grad_part
    mom_hat = new_mom / (1.0 - BETA_ONE ** ADAM_STEP)
    var_hat = new_var / (1.0 - BETA_TWO ** ADAM_STEP)
    step_dir = mom_hat / (jnp.sqrt(var_hat) + ADAM_EPS)
    new_param = param_old - LEARN_RATE * (step_dir + decay_rate * param_old)
    return new_param, new_mom, new_var, new_param.astype(jnp.bfloat16)


def reference(emb_grad, mat_grad, norm_grad, emb_param, emb_mom, emb_var, mat_param, mat_mom, mat_var, norm_param, norm_mom, norm_var):
    emb_mean = jnp.sum(emb_grad, axis=(0, 1)) / DEV_COUNT
    mat_mean = jnp.sum(mat_grad, axis=(0, 1)) / DEV_COUNT
    norm_mean = jnp.sum(norm_grad, axis=(0, 1)) / DEV_COUNT
    total_sq = jnp.sum(emb_mean * emb_mean) + jnp.sum(mat_mean * mat_mean) + jnp.sum(norm_mean * norm_mean)
    clip_scale = jnp.minimum(1.0, CLIP_NORM / jnp.sqrt(total_sq))
    emb_p, emb_m, emb_v, emb_b = adamw_update(emb_mean * clip_scale, emb_param, emb_mom, emb_var, WEIGHT_DECAY)
    mat_p, mat_m, mat_v, mat_b = adamw_update(mat_mean * clip_scale, mat_param, mat_mom, mat_var, WEIGHT_DECAY)
    norm_p, norm_m, norm_v, norm_b = adamw_update(norm_mean * clip_scale, norm_param, norm_mom, norm_var, 0.0)
    return (emb_p, emb_m, emb_v, emb_b, mat_p, mat_m, mat_v, mat_b, norm_p, norm_m, norm_v, norm_b)
```

```python
import functools

import jax
import jax.numpy as jnp
from jax import lax
from jax.experimental import pallas as pl
from jax.experimental.pallas import tpu as pltpu
from jax.sharding import PartitionSpec as P

LEARN_RATE = 0.003
BETA_ONE = 0.9
BETA_TWO = 0.95
ADAM_EPS = 1e-8
WEIGHT_DECAY = 0.1
CLIP_NORM = 1.0
ADAM_STEP = 10

MESH = pl.DeviceIdType.MESH
F32 = jnp.float32
LANES = 128
SPLIT = 2
AHEAD = 2
SLOTS = 4
LAG_ONE, LAG_TWO, LAG_SIDE, LAG_MID, LAG_BACK = 1, 2, 3, 4, 5
NORM_START, NORM_STEP = 2, 3


def adamw_update(grad_part, param_old, mom_old, var_old, decay_rate):
    new_mom = BETA_ONE * mom_old + (1.0 - BETA_ONE) * grad_part
    new_var = BETA_TWO * var_old + (1.0 - BETA_TWO) * grad_part * grad_part
    mom_hat = new_mom / (1.0 - BETA_ONE ** ADAM_STEP)
    var_hat = new_var / (1.0 - BETA_TWO ** ADAM_STEP)
    step_dir = mom_hat / (jnp.sqrt(var_hat) + ADAM_EPS)
    new_param = param_old - LEARN_RATE * (step_dir + decay_rate * param_old)
    return (new_param, new_mom, new_var, new_param.astype(jnp.bfloat16))


def reduce_kernel(inv_count, emb_ref, mat_ref, norm_ref, emb_out, mat_out, norm_out, sq_out,
                  acc, own, one, two, zin, zmid, norm_all, nsend, nown, nacc, none, ntwo, nzin, nzmid, sq_part, sq_all,
                  core_send, core_recv, own_sem, one_send, one_recv, two_send, two_recv,
                  side_send, side_recv, mid_send, mid_recv, back_send, emb_sem, mat_sem,
                  norm_sem, nsend_sem, nrecv_sem, sq_send, sq_recv):
    z = lax.axis_index("dp")
    f = lax.axis_index("fsdp")
    y, x, c = f // 4, (f // 2) % 2, f % 2
    width = acc.shape[4]
    cols = width // SPLIT
    rounds = acc.shape[3] // 8 * SPLIT
    is_end = (z == 0) | (z == 3)
    is_mid = (z == 1) | (z == 2)
    side = z + 1 - 2 * (z % 2)
    core_peer = (z, y * 4 + x * 2 + 1 - c)
    x_peer = (z, y * 4 + (1 - x) * 2 + c)
    y_peer = (z, (1 - y) * 4 + x * 2 + c)
    side_peer = (side, f)
    mid_peer = (lax.rem(3 - z, 4), f)

    def remote(src, dst, send_sem, recv_sem, peer):
        return pltpu.make_async_remote_copy(src, dst, send_sem, recv_sem, device_id=peer, device_id_type=MESH)

    def piece(q):
        return pl.ds(pl.multiple_of(lax.div(q, SPLIT) * 8, 8), 8), pl.ds(pl.multiple_of(lax.rem(q, SPLIT) * cols, LANES), cols)

    def load_own(q):
        slot = lax.rem(q, SLOTS)
        rb, cb = piece(q)

        @pl.when(q < rounds - SPLIT)
        def _():
            pltpu.make_async_copy(emb_ref.at[:, :, c, :, rb, cb], own.at[slot], own_sem.at[slot]).start()

        @pl.when(q >= rounds - SPLIT)
        def _():
            pltpu.make_async_copy(mat_ref.at[:, :, c, :, :, cb], own.at[slot], own_sem.at[slot]).start()

    norm_load = pltpu.make_async_copy(norm_ref, norm_all, norm_sem)
    norm_load.start()
    for q in range(AHEAD):
        load_own(jnp.int32(q))

    barrier = pltpu.get_barrier_semaphore()
    for step in range(1, 8):
        pl.semaphore_signal(barrier, inc=1, device_id=(z, lax.rem(f + step, 8)), device_id_type=MESH)
    pl.semaphore_signal(barrier, inc=1, device_id=side_peer, device_id_type=MESH)

    @pl.when(is_mid)
    def _():
        pl.semaphore_signal(barrier, inc=1, device_id=mid_peer, device_id_type=MESH)

        pl.semaphore_wait(barrier, 9)

    @pl.when(is_end)
    def _():
        pl.semaphore_wait(barrier, 8)

    def send_core(q, carry):
        rb, cb = piece(q)
        remote(emb_ref.at[:, :, 1 - c, :, rb, cb], acc.at[:, :, :, rb, cb], core_send, core_recv.at[q], core_peer).start()
        return carry

    lax.fori_loop(0, rounds - SPLIT, send_core, 0)
    for q in range(rounds - SPLIT, rounds):
        rb, cb = piece(jnp.int32(q))
        remote(mat_ref.at[:, :, 1 - c, :, :, cb], acc.at[:, :, :, rb, cb], core_send, core_recv.at[q], core_peer).start()

    norm_load.wait()
    shard = nacc.shape[3]
    for yy in range(2):
        for xx in range(2):
            first = norm_all[:, (4 * yy + 2 * xx) * shard:(4 * yy + 2 * xx + 1) * shard]
            second = norm_all[:, (4 * yy + 2 * xx + 1) * shard:(4 * yy + 2 * xx + 2) * shard]
            nsend[yy, xx] = jnp.where(c == 0, second, first)
            nown[yy, xx] = jnp.where(c == 0, first, second)
    sq_part[...] = jnp.zeros_like(sq_part)

    def one_copy(q, h):
        rb, cb = piece(q)
        if h == 0:
            return remote(acc.at[:, 1 - x, 0, rb, cb], one.at[0, :, rb, cb], one_send.at[0], one_recv.at[0, q], x_peer)
        return remote(acc.at[1 - y, :, 1, rb, cb], one.at[1, :, rb, cb], one_send.at[1], one_recv.at[1, q], y_peer)

    def two_copy(q, h):
        rb, cb = piece(q)
        if h == 0:
            return remote(acc.at[1 - y, x, 0, rb, cb], two.at[0, rb, cb], two_send.at[0], two_recv.at[0, q], y_peer)
        return remote(acc.at[y, 1 - x, 1, rb, cb], two.at[1, rb, cb], two_send.at[1], two_recv.at[1, q], x_peer)

    def side_copy(q):
        rb, cb = piece(q)
        return remote(acc.at[y, x, :, rb, cb], zin.at[:, rb, cb], side_send, side_recv.at[q], side_peer)

    def mid_copy(q):
        rb, cb = piece(q)
        return remote(acc.at[y, x, :, rb, cb], zmid.at[:, rb, cb], mid_send, mid_recv.at[q], mid_peer)

    def back_copy(q):
        rb, cb = piece(q)
        return remote(zin.at[:, rb, cb], zin.at[:, rb, cb], back_send, side_recv.at[q], side_peer)

    def store_out(q):
        rb, cb = piece(q)

        @pl.when(q < rounds - SPLIT)
        def _():
            pltpu.make_async_copy(zin.at[:, rb, cb], emb_out.at[:, rb, cb], emb_sem).start()

        @pl.when(q >= rounds - SPLIT)
        def _():
            pltpu.make_async_copy(zin.at[:, rb, cb], mat_out.at[:, :, cb], mat_sem).start()

    def add_squares(total):
        sq = total * total
        part = sq_part[...]
        for h in range(2):
            for j in range(cols // LANES):
                part = part + sq[h, :, j * LANES:(j + 1) * LANES]
        sq_part[...] = part

    def norm_core():
        return remote(nsend, nacc, nsend_sem.at[0], nrecv_sem.at[0], core_peer)

    def norm_one():
        return remote(nacc.at[:, 1 - x], none, nsend_sem.at[1], nrecv_sem.at[1], x_peer)

    def norm_two():
        return remote(nacc.at[1 - y, x], ntwo, nsend_sem.at[2], nrecv_sem.at[2], y_peer)

    def norm_side():
        return remote(nacc.at[y, x], nzin, nsend_sem.at[3], nrecv_sem.at[3], side_peer)

    def norm_mid():
        return remote(nacc.at[y, x], nzmid, nsend_sem.at[4], nrecv_sem.at[4], mid_peer)

    def norm_back():
        return remote(nzin, nzin, nsend_sem.at[5], nrecv_sem.at[3], side_peer)

    norm_core().start()

    def body(t, carry):
        @pl.when(t + AHEAD < rounds)
        def _():
            load_own(t + AHEAD)

        @pl.when(t < rounds)
        def _():
            rb, cb = piece(t)
            slot = lax.rem(t, SLOTS)
            pltpu.make_async_copy(own.at[slot], own.at[slot], own_sem.at[slot]).wait()
            pltpu.make_async_copy(own.at[slot], own.at[slot], core_recv.at[t]).wait()
            acc[:, :, :, rb, cb] = acc[:, :, :, rb, cb] + own[slot]
            one_copy(t, 0).start()
            one_copy(t, 1).start()

        q1 = t - LAG_ONE

        @pl.when((q1 >= 0) & (q1 < rounds))
        def _():
            rb, cb = piece(q1)
            one_copy(q1, 0).wait_recv()
            acc[:, x, 0, rb, cb] = acc[:, x, 0, rb, cb] + one[0, :, rb, cb]
            two_copy(q1, 0).start()
            one_copy(q1, 1).wait_recv()
            acc[y, :, 1, rb, cb] = acc[y, :, 1, rb, cb] + one[1, :, rb, cb]
            two_copy(q1, 1).start()

        q2 = t - LAG_TWO

        @pl.when((q2 >= 0) & (q2 < rounds))
        def _():
            rb, cb = piece(q2)
            two_copy(q2, 0).wait_recv()
            two_copy(q2, 1).wait_recv()
            acc[y, x, :, rb, cb] = acc[y, x, :, rb, cb] + two[:, rb, cb]

            @pl.when(is_end)
            def _():
                side_copy(q2).start()

        q3 = t - LAG_SIDE

        @pl.when(is_mid & (q3 >= 0) & (q3 < rounds))
        def _():
            rb, cb = piece(q3)
            side_copy(q3).wait_recv()
            acc[y, x, :, rb, cb] = acc[y, x, :, rb, cb] + zin[:, rb, cb]
            mid_copy(q3).start()

        q4 = t - LAG_MID

        @pl.when(is_mid & (q4 >= 0) & (q4 < rounds))
        def _():
            rb, cb = piece(q4)
            mid_copy(q4).wait_recv()
            total = (acc[y, x, :, rb, cb] + zmid[:, rb, cb]) * inv_count
            zin[:, rb, cb] = total
            back_copy(q4).start()
            store_out(q4)
            add_squares(total)

        q5 = t - LAG_BACK

        @pl.when(is_end & (q5 >= 0) & (q5 < rounds))
        def _():
            rb, cb = piece(q5)
            back_copy(q5).wait_recv()
            store_out(q5)
            add_squares(zin[:, rb, cb])

        @pl.when(t == NORM_START)
        def _():
            norm_core().wait_recv()
            nacc[...] = nacc[...] + nown[...]
            norm_one().start()

        @pl.when(t == NORM_START + NORM_STEP)
        def _():
            norm_one().wait_recv()
            nacc[:, x] = nacc[:, x] + none[...]
            norm_two().start()

        @pl.when(t == NORM_START + 2 * NORM_STEP)
        def _():
            norm_two().wait_recv()
            nacc[y, x] = nacc[y, x] + ntwo[...]

            @pl.when(is_end)
            def _():
                norm_side().start()

        @pl.when(is_mid & (t == NORM_START + 3 * NORM_STEP))
        def _():
            norm_side().wait_recv()
            nacc[y, x] = nacc[y, x] + nzin[...]
            norm_mid().start()

        @pl.when(is_mid & (t == NORM_START + 4 * NORM_STEP))
        def _():
            norm_mid().wait_recv()
            nzin[...] = (nacc[y, x] + nzmid[...]) * inv_count
            norm_back().start()

        @pl.when(is_end & (t == NORM_START + 5 * NORM_STEP))
        def _():
            norm_back().wait_recv()

        return carry

    lax.fori_loop(0, rounds + LAG_BACK, body, 0)

    norm_total = nzin[...]
    norm_out[...] = norm_total
    norm_sq = jnp.sum(norm_total * norm_total)
    corner = (lax.broadcasted_iota(jnp.int32, sq_part.shape, 0) == 0) & (lax.broadcasted_iota(jnp.int32, sq_part.shape, 1) == 0)
    sq_part[...] = sq_part[...] + jnp.where(corner, norm_sq, 0.0)

    for step in range(1, 8):
        remote(sq_part, sq_all.at[f], sq_send, sq_recv, (z, lax.rem(f + step, 8))).start()
    sq_all[f] = sq_part[...]
    seven = pltpu.make_async_copy(sq_all.at[pl.ds(0, 7)], sq_all.at[pl.ds(0, 7)], sq_recv)
    seven.wait()
    square = sq_all[0]
    for j in range(1, 8):
        square = square + sq_all[j]
    scale = jnp.minimum(1.0, CLIP_NORM / jnp.sqrt(jnp.broadcast_to(jnp.sum(square), square.shape)))
    sq_out[...] = scale

    pltpu.make_async_copy(sq_all.at[pl.ds(0, 7)], sq_all.at[pl.ds(0, 7)], sq_send).wait()
    pltpu.make_async_copy(acc, acc, core_send).wait()
    for h in range(2):
        pltpu.make_async_copy(one.at[h], one.at[h], one_send.at[h]).wait()
        pltpu.make_async_copy(two.at[h], two.at[h], two_send.at[h]).wait()
    norm_core().wait_send()
    norm_one().wait_send()
    norm_two().wait_send()
    pltpu.make_async_copy(emb_out, emb_out, emb_sem).wait()
    pltpu.make_async_copy(mat_out, mat_out, mat_sem).wait()

    @pl.when(is_end)
    def _():
        pltpu.make_async_copy(zin, zin, side_send).wait()
        norm_side().wait_send()

    @pl.when(is_mid)
    def _():
        pltpu.make_async_copy(zin, zin, mid_send).wait()
        pltpu.make_async_copy(zin, zin, back_send).wait()
        norm_mid().wait_send()
        norm_back().wait_send()


def solution(mesh):
    dev_count = mesh.shape["dp"] * mesh.shape["fsdp"]

    def local_step(emb_grad, mat_grad, norm_grad, emb_param, emb_mom, emb_var, mat_param, mat_mom, mat_var, norm_param, norm_mom, norm_var):
        width = emb_grad.shape[3]
        emb_half, mat_half = emb_param.shape[0] // 2, mat_param.shape[0] // 2
        count, shard = norm_param.shape
        emb_in = emb_grad.reshape(2, 2, 2, 2, emb_half, width)
        mat_in = mat_grad.reshape(2, 2, 2, 2, mat_half, width)
        norm_in = norm_grad.reshape(norm_grad.shape[2:])
        rows = emb_half + mat_half
        rounds = rows // 8 * SPLIT
        cols = width // SPLIT
        any_spec = pl.BlockSpec(memory_space=pl.ANY)
        vmem_spec = pl.BlockSpec(memory_space=pltpu.VMEM)
        dma = pltpu.SemaphoreType.DMA
        emb_mean, mat_mean, norm_mean, scale = pl.pallas_call(
            functools.partial(reduce_kernel, 1.0 / dev_count),
            out_shape=(
                jax.ShapeDtypeStruct((2, emb_half, width), F32),
                jax.ShapeDtypeStruct((2, mat_half, width), F32),
                jax.ShapeDtypeStruct((count, shard), F32),
                jax.ShapeDtypeStruct((8, LANES), F32),
            ),
            in_specs=[any_spec] * 3,
            out_specs=(any_spec, any_spec, vmem_spec, vmem_spec),
            scratch_shapes=[
                pltpu.VMEM((2, 2, 2, rows, width), F32),
                pltpu.VMEM((SLOTS, 2, 2, 2, 8, cols), F32),
                pltpu.VMEM((2, 2, rows, width), F32),
                pltpu.VMEM((2, rows, width), F32),
                pltpu.VMEM((2, rows, width), F32),
                pltpu.VMEM((2, rows, width), F32),
                pltpu.VMEM(norm_in.shape, F32),
                pltpu.VMEM((2, 2, count, shard), F32),
                pltpu.VMEM((2, 2, count, shard), F32),
                pltpu.VMEM((2, 2, count, shard), F32),
                pltpu.VMEM((2, count, shard), F32),
                pltpu.VMEM((count, shard), F32),
                pltpu.VMEM((count, shard), F32),
                pltpu.VMEM((count, shard), F32),
                pltpu.VMEM((8, LANES), F32),
                pltpu.VMEM((8, 8, LANES), F32),
                dma, dma((rounds,)), dma((SLOTS,)),
                dma((2,)), dma((2, rounds)), dma((2,)), dma((2, rounds)),
                dma, dma((rounds,)), dma, dma((rounds,)), dma,
                dma, dma,
                dma, dma((6,)), dma((6,)), dma, dma,
            ],
            compiler_params=pltpu.CompilerParams(collective_id=0, has_side_effects=True, vmem_limit_bytes=56 << 20),
            name="reduce_gradients",
        )(emb_in, mat_in, norm_in)
        clip_scale = scale[0, 0]
        emb_mean = emb_mean.reshape(emb_param.shape)
        mat_mean = mat_mean.reshape(mat_param.shape)
        emb_out = adamw_update(emb_mean * clip_scale, emb_param, emb_mom, emb_var, WEIGHT_DECAY)
        mat_out = adamw_update(mat_mean * clip_scale, mat_param, mat_mom, mat_var, WEIGHT_DECAY)
        norm_out = adamw_update(norm_mean * clip_scale, norm_param, norm_mom, norm_var, 0.0)
        return emb_out + mat_out + norm_out

    grad_spec = P("dp", "fsdp", None, None)
    row_spec = P("fsdp", None)
    col_spec = P(None, "fsdp")
    in_list = (grad_spec, grad_spec, grad_spec, row_spec, row_spec, row_spec, row_spec, row_spec, row_spec, col_spec, col_spec, col_spec)
    out_list = (row_spec, row_spec, row_spec, row_spec, row_spec, row_spec, row_spec, row_spec, col_spec, col_spec, col_spec, col_spec)
    return jax.shard_map(local_step, mesh=mesh, in_specs=in_list, out_specs=out_list, check_vma=False)
```

```python
import functools

import jax
import jax.numpy as jnp
from jax import lax
from jax.experimental import pallas as pl
from jax.experimental.pallas import tpu as pltpu
from jax.sharding import PartitionSpec as P

LEARN_RATE = 0.003
BETA_ONE = 0.9
BETA_TWO = 0.95
ADAM_EPS = 1e-8
WEIGHT_DECAY = 0.1
CLIP_NORM = 1.0
ADAM_STEP = 10

MESH = pl.DeviceIdType.MESH
F32 = jnp.float32
LANES = 128
SPLIT = 3
AHEAD = 2
SLOTS = 4
CORE_AHEAD = 4
LAG_ONE, LAG_TWO, LAG_SIDE, LAG_MID, LAG_BACK = 1, 2, 4, 6, 8
NORM_START, NORM_STEP = 2, 3


def adamw_update(grad_part, param_old, mom_old, var_old, decay_rate):
    new_mom = BETA_ONE * mom_old + (1.0 - BETA_ONE) * grad_part
    new_var = BETA_TWO * var_old + (1.0 - BETA_TWO) * grad_part * grad_part
    mom_hat = new_mom / (1.0 - BETA_ONE ** ADAM_STEP)
    var_hat = new_var / (1.0 - BETA_TWO ** ADAM_STEP)
    step_dir = mom_hat / (jnp.sqrt(var_hat) + ADAM_EPS)
    new_param = param_old - LEARN_RATE * (step_dir + decay_rate * param_old)
    return (new_param, new_mom, new_var, new_param.astype(jnp.bfloat16))


def reduce_kernel(inv_count, emb_ref, mat_ref, norm_ref, emb_out, mat_out, norm_out, sq_out,
                  acc, own, one, two, zin, zmid, norm_all, nsend, nown, nacc, none, ntwo, nzin, nzmid, sq_part, sq_all,
                  core_send, core_recv, own_sem, one_send, one_recv, two_send, two_recv,
                  side_send, side_recv, mid_send, mid_recv, back_send, emb_sem, mat_sem,
                  norm_sem, nsend_sem, nrecv_sem, sq_send, sq_recv):
    z = lax.axis_index("dp")
    f = lax.axis_index("fsdp")
    y, x, c = f // 4, (f // 2) % 2, f % 2
    width = acc.shape[4]
    cols = width // SPLIT
    rounds = acc.shape[3] // 8 * SPLIT
    is_end = (z == 0) | (z == 3)
    is_mid = (z == 1) | (z == 2)
    side = z + 1 - 2 * (z % 2)
    core_peer = (z, y * 4 + x * 2 + 1 - c)
    x_peer = (z, y * 4 + (1 - x) * 2 + c)
    y_peer = (z, (1 - y) * 4 + x * 2 + c)
    side_peer = (side, f)
    mid_peer = (lax.rem(3 - z, 4), f)

    def remote(src, dst, send_sem, recv_sem, peer):
        return pltpu.make_async_remote_copy(src, dst, send_sem, recv_sem, device_id=peer, device_id_type=MESH)

    def piece(q):
        return pl.ds(pl.multiple_of(lax.div(q, SPLIT) * 8, 8), 8), pl.ds(pl.multiple_of(lax.rem(q, SPLIT) * cols, LANES), cols)

    def load_own(q):
        slot = lax.rem(q, SLOTS)
        rb, cb = piece(q)

        @pl.when(q < rounds - SPLIT)
        def _():
            pltpu.make_async_copy(emb_ref.at[:, :, c, :, rb, cb], own.at[slot], own_sem.at[slot]).start()

        @pl.when(q >= rounds - SPLIT)
        def _():
            pltpu.make_async_copy(mat_ref.at[:, :, c, :, :, cb], own.at[slot], own_sem.at[slot]).start()

    norm_load = pltpu.make_async_copy(norm_ref, norm_all, norm_sem)
    norm_load.start()
    for q in range(AHEAD):
        load_own(jnp.int32(q))

    barrier = pltpu.get_barrier_semaphore()
    for step in range(1, 8):
        pl.semaphore_signal(barrier, inc=1, device_id=(z, lax.rem(f + step, 8)), device_id_type=MESH)
    pl.semaphore_signal(barrier, inc=1, device_id=side_peer, device_id_type=MESH)

    @pl.when(is_mid)
    def _():
        pl.semaphore_signal(barrier, inc=1, device_id=mid_peer, device_id_type=MESH)

        pl.semaphore_wait(barrier, 9)

    @pl.when(is_end)
    def _():
        pl.semaphore_wait(barrier, 8)

    def send_core(q):
        rb, cb = piece(q)

        @pl.when(q < rounds - SPLIT)
        def _():
            remote(emb_ref.at[:, :, 1 - c, :, rb, cb], acc.at[:, :, :, rb, cb], core_send, core_recv.at[q], core_peer).start()

        @pl.when(q >= rounds - SPLIT)
        def _():
            remote(mat_ref.at[:, :, 1 - c, :, :, cb], acc.at[:, :, :, rb, cb], core_send, core_recv.at[q], core_peer).start()

    for q in range(CORE_AHEAD):
        send_core(jnp.int32(q))

    norm_load.wait()
    shard = nacc.shape[3]
    for yy in range(2):
        for xx in range(2):
            first = norm_all[:, (4 * yy + 2 * xx) * shard:(4 * yy + 2 * xx + 1) * shard]
            second = norm_all[:, (4 * yy + 2 * xx + 1) * shard:(4 * yy + 2 * xx + 2) * shard]
            nsend[yy, xx] = jnp.where(c == 0, second, first)
            nown[yy, xx] = jnp.where(c == 0, first, second)
    sq_part[...] = jnp.zeros_like(sq_part)

    def one_copy(q, h):
        rb, cb = piece(q)
        if h == 0:
            return remote(acc.at[:, 1 - x, 0, rb, cb], one.at[0, :, rb, cb], one_send.at[0], one_recv.at[0, q], x_peer)
        return remote(acc.at[1 - y, :, 1, rb, cb], one.at[1, :, rb, cb], one_send.at[1], one_recv.at[1, q], y_peer)

    def two_copy(q, h):
        rb, cb = piece(q)
        if h == 0:
            return remote(acc.at[1 - y, x, 0, rb, cb], two.at[0, rb, cb], two_send.at[0], two_recv.at[0, q], y_peer)
        return remote(acc.at[y, 1 - x, 1, rb, cb], two.at[1, rb, cb], two_send.at[1], two_recv.at[1, q], x_peer)

    def side_copy(q):
        rb, cb = piece(q)
        return remote(acc.at[y, x, :, rb, cb], zin.at[:, rb, cb], side_send, side_recv.at[q], side_peer)

    def mid_copy(q):
        rb, cb = piece(q)
        return remote(acc.at[y, x, :, rb, cb], zmid.at[:, rb, cb], mid_send, mid_recv.at[q], mid_peer)

    def back_copy(q):
        rb, cb = piece(q)
        return remote(zin.at[:, rb, cb], zin.at[:, rb, cb], back_send, side_recv.at[q], side_peer)

    def store_out(q):
        rb, cb = piece(q)

        @pl.when(q < rounds - SPLIT)
        def _():
            pltpu.make_async_copy(zin.at[:, rb, cb], emb_out.at[:, rb, cb], emb_sem).start()

        @pl.when(q >= rounds - SPLIT)
        def _():
            pltpu.make_async_copy(zin.at[:, rb, cb], mat_out.at[:, :, cb], mat_sem).start()

    def add_squares(total):
        sq = total * total
        part = sq_part[...]
        for h in range(2):
            for j in range(cols // LANES):
                part = part + sq[h, :, j * LANES:(j + 1) * LANES]
        sq_part[...] = part

    def norm_core():
        return remote(nsend, nacc, nsend_sem.at[0], nrecv_sem.at[0], core_peer)

    def norm_one():
        return remote(nacc.at[:, 1 - x], none, nsend_sem.at[1], nrecv_sem.at[1], x_peer)

    def norm_two():
        return remote(nacc.at[1 - y, x], ntwo, nsend_sem.at[2], nrecv_sem.at[2], y_peer)

    def norm_side():
        return remote(nacc.at[y, x], nzin, nsend_sem.at[3], nrecv_sem.at[3], side_peer)

    def norm_mid():
        return remote(nacc.at[y, x], nzmid, nsend_sem.at[4], nrecv_sem.at[4], mid_peer)

    def norm_back():
        return remote(nzin, nzin, nsend_sem.at[5], nrecv_sem.at[3], side_peer)

    norm_core().start()

    def body(t, carry):
        @pl.when(t + CORE_AHEAD < rounds)
        def _():
            send_core(t + CORE_AHEAD)

        @pl.when(t + AHEAD < rounds)
        def _():
            load_own(t + AHEAD)

        @pl.when(t < rounds)
        def _():
            rb, cb = piece(t)
            slot = lax.rem(t, SLOTS)
            pltpu.make_async_copy(own.at[slot], own.at[slot], own_sem.at[slot]).wait()
            pltpu.make_async_copy(own.at[slot], own.at[slot], core_recv.at[t]).wait()
            acc[:, :, :, rb, cb] = acc[:, :, :, rb, cb] + own[slot]
            one_copy(t, 0).start()
            one_copy(t, 1).start()

        q1 = t - LAG_ONE

        @pl.when((q1 >= 0) & (q1 < rounds))
        def _():
            rb, cb = piece(q1)
            one_copy(q1, 0).wait_recv()
            acc[:, x, 0, rb, cb] = acc[:, x, 0, rb, cb] + one[0, :, rb, cb]
            two_copy(q1, 0).start()
            one_copy(q1, 1).wait_recv()
            acc[y, :, 1, rb, cb] = acc[y, :, 1, rb, cb] + one[1, :, rb, cb]
            two_copy(q1, 1).start()

        q2 = t - LAG_TWO

        @pl.when((q2 >= 0) & (q2 < rounds))
        def _():
            rb, cb = piece(q2)
            two_copy(q2, 0).wait_recv()
            two_copy(q2, 1).wait_recv()
            acc[y, x, :, rb, cb] = acc[y, x, :, rb, cb] + two[:, rb, cb]

            @pl.when(is_end)
            def _():
                side_copy(q2).start()

        q3 = t - LAG_SIDE

        @pl.when(is_mid & (q3 >= 0) & (q3 < rounds))
        def _():
            rb, cb = piece(q3)
            side_copy(q3).wait_recv()
            acc[y, x, :, rb, cb] = acc[y, x, :, rb, cb] + zin[:, rb, cb]
            mid_copy(q3).start()

        q4 = t - LAG_MID

        @pl.when(is_mid & (q4 >= 0) & (q4 < rounds))
        def _():
            rb, cb = piece(q4)
            mid_copy(q4).wait_recv()
            total = (acc[y, x, :, rb, cb] + zmid[:, rb, cb]) * inv_count
            zin[:, rb, cb] = total
            back_copy(q4).start()
            store_out(q4)
            add_squares(total)

        q5 = t - LAG_BACK

        @pl.when(is_end & (q5 >= 0) & (q5 < rounds))
        def _():
            rb, cb = piece(q5)
            back_copy(q5).wait_recv()
            store_out(q5)
            add_squares(zin[:, rb, cb])

        @pl.when(t == NORM_START)
        def _():
            norm_core().wait_recv()
            nacc[...] = nacc[...] + nown[...]
            norm_one().start()

        @pl.when(t == NORM_START + NORM_STEP)
        def _():
            norm_one().wait_recv()
            nacc[:, x] = nacc[:, x] + none[...]
            norm_two().start()

        @pl.when(t == NORM_START + 2 * NORM_STEP)
        def _():
            norm_two().wait_recv()
            nacc[y, x] = nacc[y, x] + ntwo[...]

            @pl.when(is_end)
            def _():
                norm_side().start()

        @pl.when(is_mid & (t == NORM_START + 3 * NORM_STEP))
        def _():
            norm_side().wait_recv()
            nacc[y, x] = nacc[y, x] + nzin[...]
            norm_mid().start()

        @pl.when(is_mid & (t == NORM_START + 4 * NORM_STEP))
        def _():
            norm_mid().wait_recv()
            nzin[...] = (nacc[y, x] + nzmid[...]) * inv_count
            norm_back().start()

        @pl.when(is_end & (t == NORM_START + 5 * NORM_STEP))
        def _():
            norm_back().wait_recv()

        return carry

    lax.fori_loop(0, rounds + LAG_BACK, body, 0)

    norm_total = nzin[...]
    norm_out[...] = norm_total
    norm_sq = jnp.sum(norm_total * norm_total)
    corner = (lax.broadcasted_iota(jnp.int32, sq_part.shape, 0) == 0) & (lax.broadcasted_iota(jnp.int32, sq_part.shape, 1) == 0)
    sq_part[...] = sq_part[...] + jnp.where(corner, norm_sq, 0.0)

    for step in range(1, 8):
        remote(sq_part, sq_all.at[f], sq_send, sq_recv, (z, lax.rem(f + step, 8))).start()
    sq_all[f] = sq_part[...]
    seven = pltpu.make_async_copy(sq_all.at[pl.ds(0, 7)], sq_all.at[pl.ds(0, 7)], sq_recv)
    seven.wait()
    square = sq_all[0]
    for j in range(1, 8):
        square = square + sq_all[j]
    scale = jnp.minimum(1.0, CLIP_NORM / jnp.sqrt(jnp.broadcast_to(jnp.sum(square), square.shape)))
    sq_out[...] = scale

    pltpu.make_async_copy(sq_all.at[pl.ds(0, 7)], sq_all.at[pl.ds(0, 7)], sq_send).wait()
    pltpu.make_async_copy(acc, acc, core_send).wait()
    for h in range(2):
        pltpu.make_async_copy(one.at[h], one.at[h], one_send.at[h]).wait()
        pltpu.make_async_copy(two.at[h], two.at[h], two_send.at[h]).wait()
    norm_core().wait_send()
    norm_one().wait_send()
    norm_two().wait_send()
    pltpu.make_async_copy(emb_out, emb_out, emb_sem).wait()
    pltpu.make_async_copy(mat_out, mat_out, mat_sem).wait()

    @pl.when(is_end)
    def _():
        pltpu.make_async_copy(zin, zin, side_send).wait()
        norm_side().wait_send()

    @pl.when(is_mid)
    def _():
        pltpu.make_async_copy(zin, zin, mid_send).wait()
        pltpu.make_async_copy(zin, zin, back_send).wait()
        norm_mid().wait_send()
        norm_back().wait_send()


def solution(mesh):
    dev_count = mesh.shape["dp"] * mesh.shape["fsdp"]

    def local_step(emb_grad, mat_grad, norm_grad, emb_param, emb_mom, emb_var, mat_param, mat_mom, mat_var, norm_param, norm_mom, norm_var):
        width = emb_grad.shape[3]
        emb_half, mat_half = emb_param.shape[0] // 2, mat_param.shape[0] // 2
        count, shard = norm_param.shape
        emb_in = emb_grad.reshape(2, 2, 2, 2, emb_half, width)
        mat_in = mat_grad.reshape(2, 2, 2, 2, mat_half, width)
        norm_in = norm_grad.reshape(norm_grad.shape[2:])
        rows = emb_half + mat_half
        rounds = rows // 8 * SPLIT
        cols = width // SPLIT
        any_spec = pl.BlockSpec(memory_space=pl.ANY)
        vmem_spec = pl.BlockSpec(memory_space=pltpu.VMEM)
        dma = pltpu.SemaphoreType.DMA
        emb_mean, mat_mean, norm_mean, scale = pl.pallas_call(
            functools.partial(reduce_kernel, 1.0 / dev_count),
            out_shape=(
                jax.ShapeDtypeStruct((2, emb_half, width), F32),
                jax.ShapeDtypeStruct((2, mat_half, width), F32),
                jax.ShapeDtypeStruct((count, shard), F32),
                jax.ShapeDtypeStruct((8, LANES), F32),
            ),
            in_specs=[any_spec] * 3,
            out_specs=(any_spec, any_spec, vmem_spec, vmem_spec),
            scratch_shapes=[
                pltpu.VMEM((2, 2, 2, rows, width), F32),
                pltpu.VMEM((SLOTS, 2, 2, 2, 8, cols), F32),
                pltpu.VMEM((2, 2, rows, width), F32),
                pltpu.VMEM((2, rows, width), F32),
                pltpu.VMEM((2, rows, width), F32),
                pltpu.VMEM((2, rows, width), F32),
                pltpu.VMEM(norm_in.shape, F32),
                pltpu.VMEM((2, 2, count, shard), F32),
                pltpu.VMEM((2, 2, count, shard), F32),
                pltpu.VMEM((2, 2, count, shard), F32),
                pltpu.VMEM((2, count, shard), F32),
                pltpu.VMEM((count, shard), F32),
                pltpu.VMEM((count, shard), F32),
                pltpu.VMEM((count, shard), F32),
                pltpu.VMEM((8, LANES), F32),
                pltpu.VMEM((8, 8, LANES), F32),
                dma, dma((rounds,)), dma((SLOTS,)),
                dma((2,)), dma((2, rounds)), dma((2,)), dma((2, rounds)),
                dma, dma((rounds,)), dma, dma((rounds,)), dma,
                dma, dma,
                dma, dma((6,)), dma((6,)), dma, dma,
            ],
            compiler_params=pltpu.CompilerParams(collective_id=0, has_side_effects=True, vmem_limit_bytes=56 << 20),
            name="reduce_gradients",
        )(emb_in, mat_in, norm_in)
        clip_scale = scale[0, 0]
        emb_mean = emb_mean.reshape(emb_param.shape)
        mat_mean = mat_mean.reshape(mat_param.shape)
        emb_out = adamw_update(emb_mean * clip_scale, emb_param, emb_mom, emb_var, WEIGHT_DECAY)
        mat_out = adamw_update(mat_mean * clip_scale, mat_param, mat_mom, mat_var, WEIGHT_DECAY)
        norm_out = adamw_update(norm_mean * clip_scale, norm_param, norm_mom, norm_var, 0.0)
        return emb_out + mat_out + norm_out

    grad_spec = P("dp", "fsdp", None, None)
    row_spec = P("fsdp", None)
    col_spec = P(None, "fsdp")
    in_list = (grad_spec, grad_spec, grad_spec, row_spec, row_spec, row_spec, row_spec, row_spec, row_spec, col_spec, col_spec, col_spec)
    out_list = (row_spec, row_spec, row_spec, row_spec, row_spec, row_spec, row_spec, row_spec, col_spec, col_spec, col_spec, col_spec)
    return jax.shard_map(local_step, mesh=mesh, in_specs=in_list, out_specs=out_list, check_vma=False)
```

```python
import functools

import jax
import jax.numpy as jnp
from jax import lax
from jax.experimental import pallas as pl
from jax.experimental.pallas import tpu as pltpu
from jax.sharding import PartitionSpec as P

LEARN_RATE = 0.003
BETA_ONE = 0.9
BETA_TWO = 0.95
ADAM_EPS = 1e-8
WEIGHT_DECAY = 0.1
CLIP_NORM = 1.0
ADAM_STEP = 10

MESH = pl.DeviceIdType.MESH
F32 = jnp.float32
LANES = 128
SPLIT = 2
AHEAD = 2
SLOTS = 4
CORE_AHEAD = 4
LAG_ONE, LAG_TWO, LAG_SIDE, LAG_MID, LAG_BACK = 2, 4, 6, 8, 10
NORM_START, NORM_STEP = 4, 6
LINE_BLOCKS = 4
LINE_SPLIT = 3
LINE_RATE, LINE_STEP = 4, 2
ADAM_ROWS = 32
VMEM_MIB = 52


def reduce_kernel(inv_count, emb_ref, mat_ref, norm_ref, emb_out, mat_out, norm_out, scale_out,
                  acc, own, one, two, zin, zmid, lown, lside, lmid, lback, lone, ltwo,
                  norm_all, nsend, nown, nacc, none, ntwo, nzin, nzmid, sq_main, sq_line, sq_all,
                  core_send, core_recv, own_sem, one_send, one_recv, two_send, two_recv,
                  side_send, side_recv, mid_send, mid_recv, back_send, emb_sem, mat_sem,
                  lown_sem, line_send, line_recv, norm_sem, nsend_sem, nrecv_sem, sq_send, sq_recv):
    z = lax.axis_index("dp")
    f = lax.axis_index("fsdp")
    y, x, c = f // 4, (f // 2) % 2, f % 2
    width = acc.shape[3]
    half = width // 2
    cols = half // SPLIT
    emb_blocks = emb_ref.shape[3] // 8
    rounds = one.shape[2] // 8 * SPLIT
    emb_rounds = (emb_blocks - LINE_BLOCKS) * SPLIT
    lines = lown.shape[0]
    lwidth = width // LINE_SPLIT
    quarter = lwidth // 4
    is_end = (z == 0) | (z == 3)
    is_mid = (z == 1) | (z == 2)
    high = z // 2
    side = z + 1 - 2 * (z % 2)
    core_peer = (z, y * 4 + x * 2 + 1 - c)
    x_peer = (z, y * 4 + (1 - x) * 2 + c)
    y_peer = (z, (1 - y) * 4 + x * 2 + c)
    side_peer = (side, f)
    mid_peer = (lax.rem(3 - z, 4), f)

    def remote(src, dst, send_sem, recv_sem, peer):
        return pltpu.make_async_remote_copy(src, dst, send_sem, recv_sem, device_id=peer, device_id_type=MESH)

    def take(ref, sem):
        pltpu.make_async_copy(ref, ref, sem).wait()

    def piece(q):
        block, sub = lax.div(q, SPLIT), lax.rem(q, SPLIT) * cols
        rows = pl.ds(pl.multiple_of((block + LINE_BLOCKS) * 8, 8), 8)
        inner = pl.ds(pl.multiple_of(block * 8, 8), 8)
        wide = [pl.ds(pl.multiple_of(sub + h * half, LANES), cols) for h in range(2)]
        return rows, inner, wide, pl.ds(pl.multiple_of(sub, LANES), cols)

    def mat_rows(q):
        return pl.ds(pl.multiple_of((lax.div(q, SPLIT) + LINE_BLOCKS - emb_blocks) * 8, 8), 8)

    def from_emb_or_mat(q, do):
        rows, _, wide, _ = piece(q)

        @pl.when(q < emb_rounds)
        def _():
            for h in range(2):
                do(emb_ref, rows, h, wide[h])

        @pl.when(q >= emb_rounds)
        def _():
            for h in range(2):
                do(mat_ref, mat_rows(q), h, wide[h])

    def load_own(q):
        slot = lax.rem(q, SLOTS)
        from_emb_or_mat(q, lambda ref, rows, h, cs: pltpu.make_async_copy(
            ref.at[:, :, c, rows, cs], own.at[slot, h], own_sem.at[slot]).start())

    def send_core(q):
        rb = piece(q)[0]
        from_emb_or_mat(q, lambda ref, rows, h, cs: remote(
            ref.at[:, :, 1 - c, rows, cs], acc.at[:, :, rb, cs], core_send, core_recv.at[q], core_peer).start())

    def line_at(i, start=0, size=4):
        rows = pl.ds(pl.multiple_of(lax.div(i, LINE_SPLIT) * 8, 8), 8)
        return rows, pl.ds(pl.multiple_of(lax.rem(i, LINE_SPLIT) * lwidth + start * quarter, LANES), size * quarter)

    def load_line(i):
        rows, cs = line_at(i)
        return pltpu.make_async_copy(emb_ref.at[:, :, c, rows, cs], lown.at[i], lown_sem.at[i])

    def line_core(i):
        rows, cs = line_at(i)
        return remote(emb_ref.at[:, :, 1 - c, rows, cs], acc.at[:, :, rows, cs], line_send.at[0], line_recv.at[0, i], core_peer)

    norm_load = pltpu.make_async_copy(norm_ref, norm_all, norm_sem)
    norm_load.start()
    for q in range(AHEAD):
        load_own(jnp.int32(q))
    for i in range(lines):
        load_line(jnp.int32(i)).start()

    barrier = pltpu.get_barrier_semaphore()
    for step in range(1, 8):
        pl.semaphore_signal(barrier, inc=1, device_id=(z, lax.rem(f + step, 8)), device_id_type=MESH)
    pl.semaphore_signal(barrier, inc=1, device_id=side_peer, device_id_type=MESH)

    @pl.when(is_mid)
    def _():
        pl.semaphore_signal(barrier, inc=1, device_id=mid_peer, device_id_type=MESH)
        pl.semaphore_wait(barrier, 9)

    @pl.when(is_end)
    def _():
        pl.semaphore_wait(barrier, 8)

    for q in range(CORE_AHEAD):
        if q % LINE_RATE == 0:
            line_core(jnp.int32(q // LINE_RATE)).start()
        send_core(jnp.int32(q))

    norm_load.wait()
    shard = nacc.shape[4]
    for yy in range(2):
        for xx in range(2):
            at = (4 * yy + 2 * xx) * shard
            first = norm_all[:, :, at:at + shard]
            second = norm_all[:, :, at + shard:at + 2 * shard]
            nsend[yy, xx] = jnp.where(c == 0, second, first)
            nown[yy, xx] = jnp.where(c == 0, first, second)
    sq_main[...] = jnp.zeros_like(sq_main)
    sq_line[...] = jnp.zeros_like(sq_line)

    def one_copy(q, h):
        rb, inner, wide, cs = piece(q)
        src = acc.at[:, 1 - x, rb, wide[0]] if h == 0 else acc.at[1 - y, :, rb, wide[1]]
        return remote(src, one.at[h, :, inner, cs], one_send.at[h], one_recv.at[h, q], (x_peer, y_peer)[h])

    def two_copy(q, h):
        rb, inner, wide, cs = piece(q)
        src = acc.at[1 - y, x, rb, wide[0]] if h == 0 else acc.at[y, 1 - x, rb, wide[1]]
        return remote(src, two.at[h, inner, cs], two_send.at[h], two_recv.at[h, q], (y_peer, x_peer)[h])

    def side_start(q):
        rb, _, wide, _ = piece(q)
        for cs in wide:
            remote(acc.at[y, x, rb, cs], zin.at[rb, cs], side_send, side_recv.at[q], side_peer).start()

    def mid_start(q):
        rb, inner, wide, _ = piece(q)
        for cs in wide:
            remote(acc.at[y, x, rb, cs], zmid.at[inner, cs], mid_send, mid_recv.at[q], mid_peer).start()

    def back_start(q):
        rb, _, wide, _ = piece(q)
        for cs in wide:
            remote(zin.at[rb, cs], zin.at[rb, cs], back_send, side_recv.at[q], side_peer).start()

    def both(q):
        _, inner, _, cs = piece(q)
        return two.at[:, inner, cs]

    def store_out(q):
        rb, _, wide, _ = piece(q)

        @pl.when(q < emb_rounds)
        def _():
            for cs in wide:
                pltpu.make_async_copy(zin.at[rb, cs], emb_out.at[rb, cs], emb_sem).start()

        @pl.when(q >= emb_rounds)
        def _():
            for cs in wide:
                pltpu.make_async_copy(zin.at[rb, cs], mat_out.at[mat_rows(q), cs], mat_sem).start()

    def add_squares(part_ref, total):
        sq = total * total
        part = part_ref[...]
        for j in range(total.shape[1] // LANES):
            part = part + sq[:, j * LANES:(j + 1) * LANES]
        part_ref[...] = part

    def line_side(i):
        rows, cs = line_at(i, 1 - high, 3)
        return remote(acc.at[:, :, rows, cs], lside.at[i], line_send.at[1], line_recv.at[1, i], side_peer)

    def line_mid(i):
        rows, cs = line_at(i, 2 - 2 * high, 2)
        return remote(acc.at[:, :, rows, cs], lmid.at[i], line_send.at[2], line_recv.at[2, i], mid_peer)

    def line_back(i):
        rows, cs = line_at(i, 3 * high, 1)
        return remote(acc.at[:, :, rows, cs], lback.at[i], line_send.at[3], line_recv.at[3, i], side_peer)

    def line_one(i, h):
        rows, cs = line_at(i, z, 1)
        src = acc.at[:, 1 - x, rows, cs] if h == 0 else acc.at[1 - y, :, rows, cs]
        return remote(src, lone.at[i], line_send.at[4], line_recv.at[4, i], (x_peer, y_peer)[h])

    def line_two(i, h):
        rows, cs = line_at(i, z, 1)
        src = acc.at[1 - y, x, rows, cs] if h == 0 else acc.at[y, 1 - x, rows, cs]
        return remote(src, ltwo.at[i], line_send.at[5], line_recv.at[5, i], (y_peer, x_peer)[h])

    def gather_side(i):
        rows, cs = line_at(i, 3 * high, 1)
        return remote(zin.at[rows, cs], zin.at[rows, cs], line_send.at[6], line_recv.at[6, i], side_peer)

    def gather_mid(i):
        rows, cs = line_at(i, 2 * high, 2)
        return remote(zin.at[rows, cs], zin.at[rows, cs], line_send.at[7], line_recv.at[7, i], mid_peer)

    def gather_back(i):
        rows, cs = line_at(i, 1 - high, 3)
        return remote(zin.at[rows, cs], zin.at[rows, cs], line_send.at[8], line_recv.at[8, i], side_peer)

    def line_out(i):
        rows, cs = line_at(i)
        pltpu.make_async_copy(zin.at[rows, cs], emb_out.at[rows, cs], emb_sem).start()
        add_squares(sq_line, zin[rows, cs])

    def either_way(i, do):
        @pl.when(lax.rem(i, 2) == 0)
        def _():
            do(0)

        @pl.when(lax.rem(i, 2) == 1)
        def _():
            do(1)

    def line_stage_0(i):
        rows, cs = line_at(i)
        load_line(i).wait()
        take(lown.at[i], line_recv.at[0, i])
        acc[:, :, rows, cs] = acc[:, :, rows, cs] + lown[i]

        @pl.when(is_end)
        def _():
            line_side(i).start()

    def line_stage_1(i):
        @pl.when(is_mid)
        def _():
            rows, cs = line_at(i, 1 - high, 3)
            take(lside.at[i], line_recv.at[1, i])
            acc[:, :, rows, cs] = acc[:, :, rows, cs] + lside[i]
            line_mid(i).start()

    def line_stage_2(i):
        @pl.when(is_mid)
        def _():
            rows, cs = line_at(i, 2 * high, 2)
            take(lmid.at[i], line_recv.at[2, i])
            acc[:, :, rows, cs] = acc[:, :, rows, cs] + lmid[i]
            line_back(i).start()

    def line_stage_3(i):
        @pl.when(is_end)
        def _():
            rows, cs = line_at(i, 3 * high, 1)
            take(lback.at[i], line_recv.at[3, i])
            acc[:, :, rows, cs] = acc[:, :, rows, cs] + lback[i]

        either_way(i, lambda h: line_one(i, h).start())

    def line_stage_4(i):
        rows, cs = line_at(i, z, 1)
        take(lone.at[i], line_recv.at[4, i])

        def add(h):
            if h == 0:
                acc[:, x, rows, cs] = acc[:, x, rows, cs] + lone[i]
            else:
                acc[y, :, rows, cs] = acc[y, :, rows, cs] + lone[i]
            line_two(i, h).start()

        either_way(i, add)

    def line_stage_5(i):
        rows, cs = line_at(i, z, 1)
        take(ltwo.at[i], line_recv.at[5, i])
        zin[rows, cs] = (acc[y, x, rows, cs] + ltwo[i]) * inv_count

        @pl.when(is_end)
        def _():
            gather_side(i).start()

    def line_stage_6(i):
        @pl.when(is_mid)
        def _():
            take(ltwo.at[i], line_recv.at[6, i])
            gather_mid(i).start()

    def line_stage_7(i):
        @pl.when(is_mid)
        def _():
            take(lone.at[i], line_recv.at[7, i])
            gather_back(i).start()
            line_out(i)

    def line_stage_8(i):
        @pl.when(is_end)
        def _():
            take(lside.at[i, 0, 0], line_recv.at[8, i])
            line_out(i)

    line_stages = (line_stage_0, line_stage_1, line_stage_2, line_stage_3, line_stage_4, line_stage_5, line_stage_6,
                   line_stage_7, line_stage_8)

    norm_core = remote(nsend, nacc, nsend_sem.at[0], nrecv_sem.at[0], core_peer)
    norm_one = remote(nacc.at[:, 1 - x], none, nsend_sem.at[1], nrecv_sem.at[1], x_peer)
    norm_two = remote(nacc.at[1 - y, x], ntwo, nsend_sem.at[2], nrecv_sem.at[2], y_peer)
    norm_side = remote(nacc.at[y, x], nzin, nsend_sem.at[3], nrecv_sem.at[3], side_peer)
    norm_mid = remote(nacc.at[y, x], nzmid, nsend_sem.at[4], nrecv_sem.at[4], mid_peer)
    norm_back = remote(nzin, nzin, nsend_sem.at[5], nrecv_sem.at[3], side_peer)
    norm_core.start()

    def body(t, carry):
        @pl.when(t + CORE_AHEAD < rounds)
        def _():
            send_core(t + CORE_AHEAD)

        @pl.when(t + AHEAD < rounds)
        def _():
            load_own(t + AHEAD)

        early = t + CORE_AHEAD

        @pl.when((lax.rem(early, LINE_RATE) == 0) & (early < lines * LINE_RATE))
        def _():
            line_core(lax.div(early, LINE_RATE)).start()

        @pl.when(t < rounds)
        def _():
            rb, _, wide, _ = piece(t)
            slot = lax.rem(t, SLOTS)
            take(own.at[slot], own_sem.at[slot])
            take(own.at[slot], core_recv.at[t])
            for h in range(2):
                acc[:, :, rb, wide[h]] = acc[:, :, rb, wide[h]] + own[slot, h]
                one_copy(t, h).start()

        q1 = t - LAG_ONE

        @pl.when((q1 >= 0) & (q1 < rounds))
        def _():
            rb, inner, wide, cs = piece(q1)
            one_copy(q1, 0).wait_recv()
            acc[:, x, rb, wide[0]] = acc[:, x, rb, wide[0]] + one[0, :, inner, cs]
            two_copy(q1, 0).start()
            one_copy(q1, 1).wait_recv()
            acc[y, :, rb, wide[1]] = acc[y, :, rb, wide[1]] + one[1, :, inner, cs]
            two_copy(q1, 1).start()

        q2 = t - LAG_TWO

        @pl.when((q2 >= 0) & (q2 < rounds))
        def _():
            rb, inner, wide, cs = piece(q2)
            for h in range(2):
                two_copy(q2, h).wait_recv()
                acc[y, x, rb, wide[h]] = acc[y, x, rb, wide[h]] + two[h, inner, cs]

            @pl.when(is_end)
            def _():
                side_start(q2)

        q3 = t - LAG_SIDE

        @pl.when(is_mid & (q3 >= 0) & (q3 < rounds))
        def _():
            rb, _, wide, _ = piece(q3)
            take(both(q3), side_recv.at[q3])
            for cs in wide:
                acc[y, x, rb, cs] = acc[y, x, rb, cs] + zin[rb, cs]
            mid_start(q3)

        q4 = t - LAG_MID

        @pl.when(is_mid & (q4 >= 0) & (q4 < rounds))
        def _():
            rb, inner, wide, _ = piece(q4)
            take(both(q4), mid_recv.at[q4])
            for cs in wide:
                total = (acc[y, x, rb, cs] + zmid[inner, cs]) * inv_count
                zin[rb, cs] = total
                add_squares(sq_main, total)
            back_start(q4)
            store_out(q4)

        q5 = t - LAG_BACK

        @pl.when(is_end & (q5 >= 0) & (q5 < rounds))
        def _():
            rb, _, wide, _ = piece(q5)
            take(both(q5), side_recv.at[q5])
            store_out(q5)
            for cs in wide:
                add_squares(sq_main, zin[rb, cs])

        for k, stage in enumerate(line_stages):
            late = t - k * LINE_STEP

            @pl.when((late >= 0) & (late < lines * LINE_RATE) & (lax.rem(late, LINE_RATE) == 0))
            def _(late=late, stage=stage):
                stage(lax.div(late, LINE_RATE))

        @pl.when(t == NORM_START)
        def _():
            norm_core.wait_recv()
            nacc[...] = nacc[...] + nown[...]
            norm_one.start()

        @pl.when(t == NORM_START + NORM_STEP)
        def _():
            norm_one.wait_recv()
            nacc[:, x] = nacc[:, x] + none[...]
            norm_two.start()

        @pl.when(t == NORM_START + 2 * NORM_STEP)
        def _():
            norm_two.wait_recv()
            nacc[y, x] = nacc[y, x] + ntwo[...]

            @pl.when(is_end)
            def _():
                norm_side.start()

        @pl.when(is_mid & (t == NORM_START + 3 * NORM_STEP))
        def _():
            norm_side.wait_recv()
            nacc[y, x] = nacc[y, x] + nzin[...]
            norm_mid.start()

        @pl.when(is_mid & (t == NORM_START + 4 * NORM_STEP))
        def _():
            norm_mid.wait_recv()
            nzin[...] = (nacc[y, x] + nzmid[...]) * inv_count
            norm_back.start()

        @pl.when(is_end & (t == NORM_START + 5 * NORM_STEP))
        def _():
            norm_back.wait_recv()

        @pl.when(t == NORM_START + 6 * NORM_STEP)
        def _():
            for j in range(norm_out.shape[0]):
                norm_out[j:j + 1, :] = nzin[j]
            norm_total = nzin[...]
            norm_sq = jnp.sum(norm_total * norm_total)
            corner = [lax.broadcasted_iota(jnp.int32, sq_line.shape, d) == 0 for d in range(2)]
            sq_norm = jnp.where(corner[0] & corner[1], norm_sq, 0.0)
            sq_all[0] = sq_norm

        return carry

    lax.fori_loop(0, rounds + LAG_BACK, body, 0)

    sq_main[...] = sq_main[...] + sq_line[...] + sq_all[0]
    for step in range(1, 8):
        remote(sq_main, sq_all.at[1 + f], sq_send, sq_recv, (z, lax.rem(f + step, 8))).start()
    sq_all[1 + f] = sq_main[...]
    seven = sq_all.at[pl.ds(0, 7)]
    take(seven, sq_recv)
    square = sq_all[1]
    for j in range(2, 9):
        square = square + sq_all[j]
    scale_out[...] = jnp.minimum(1.0, CLIP_NORM / jnp.sqrt(jnp.broadcast_to(jnp.sum(square), square.shape)))

    take(seven, sq_send)
    take(acc.at[:, :, pl.ds(0, one.shape[2])], core_send)
    for h in range(2):
        take(one.at[h], one_send.at[h])
        take(two.at[h], two_send.at[h])
    take(lown, line_send.at[0])
    take(lone, line_send.at[4])
    take(ltwo, line_send.at[5])
    norm_core.wait_send()
    norm_one.wait_send()
    norm_two.wait_send()
    take(emb_out, emb_sem)
    take(mat_out, mat_sem)

    @pl.when(is_end)
    def _():
        take(zmid, side_send)
        take(lside, line_send.at[1])
        take(ltwo, line_send.at[6])
        norm_side.wait_send()

    @pl.when(is_mid)
    def _():
        take(zmid, mid_send)
        take(zmid, back_send)
        take(lmid, line_send.at[2])
        take(lback, line_send.at[3])
        take(lone, line_send.at[7])
        take(lside.at[:, 0, 0], line_send.at[8])
        norm_mid.wait_send()
        norm_back.wait_send()


def adam_kernel(scale_ref, *refs):
    ins, outs = refs[:12], refs[12:]
    clip = scale_ref[0:1, 0:1]
    bias_one = 1.0 / (1.0 - BETA_ONE ** ADAM_STEP)
    bias_two = 1.0 / (1.0 - BETA_TWO ** ADAM_STEP)

    def update(group, rows, decay_rate):
        grad, param, mom, var = (ref[rows, :] for ref in ins[4 * group:4 * group + 4])
        grad = grad * clip
        new_mom = BETA_ONE * mom + (1.0 - BETA_ONE) * grad
        new_var = BETA_TWO * var + (1.0 - BETA_TWO) * grad * grad
        step_dir = new_mom * bias_one / (jnp.sqrt(new_var * bias_two) + ADAM_EPS)
        new_param = param - LEARN_RATE * (step_dir + decay_rate * param)
        for ref, value in zip(outs[4 * group:4 * group + 4], (new_param, new_mom, new_var, new_param)):
            ref[rows, :] = value.astype(ref.dtype)

    @pl.when(pl.program_id(0) == 0)
    def _():
        update(2, slice(0, ins[8].shape[0]), 0.0)
        for r in range(0, ins[4].shape[0], 8):
            update(1, slice(r, r + 8), WEIGHT_DECAY)

    def rows_of(r, carry):
        update(0, pl.ds(pl.multiple_of(r * 8, 8), 8), WEIGHT_DECAY)
        return carry

    lax.fori_loop(0, ins[0].shape[0] // 8, rows_of, 0)


def solution(mesh):
    dev_count = mesh.shape["dp"] * mesh.shape["fsdp"]

    def local_step(emb_grad, mat_grad, norm_grad, emb_param, emb_mom, emb_var, mat_param, mat_mom, mat_var, norm_param, norm_mom, norm_var):
        width = emb_grad.shape[3]
        emb_rows, mat_rows = emb_param.shape[0], mat_param.shape[0]
        count, shard = norm_param.shape
        emb_in = emb_grad.reshape(2, 2, 2, emb_rows, width)
        mat_in = mat_grad.reshape(2, 2, 2, mat_rows, width)
        norm_in = norm_grad.reshape(count, 1, norm_grad.shape[3])
        rows = emb_rows + mat_rows
        main_rows = rows - 8 * LINE_BLOCKS
        rounds = main_rows // 8 * SPLIT
        half = width // 2
        lines = LINE_BLOCKS * LINE_SPLIT
        quarter = width // LINE_SPLIT // 4
        any_spec = pl.BlockSpec(memory_space=pl.ANY)
        vmem_spec = pl.BlockSpec(memory_space=pltpu.VMEM)
        dma = pltpu.SemaphoreType.DMA
        vmem = lambda *shape: pltpu.VMEM(shape, F32)
        emb_mean, mat_mean, norm_mean, scale = pl.pallas_call(
            functools.partial(reduce_kernel, 1.0 / dev_count),
            out_shape=(
                jax.ShapeDtypeStruct((emb_rows, width), F32),
                jax.ShapeDtypeStruct((mat_rows, width), F32),
                jax.ShapeDtypeStruct((count, shard), F32),
                jax.ShapeDtypeStruct((8, LANES), F32),
            ),
            in_specs=[any_spec] * 3,
            out_specs=(any_spec, any_spec, vmem_spec, vmem_spec),
            scratch_shapes=[
                vmem(2, 2, rows, width),
                vmem(SLOTS, 2, 2, 2, 8, half // SPLIT),
                vmem(2, 2, main_rows, half),
                vmem(2, main_rows, half),
                vmem(rows, width),
                vmem(main_rows, width),
                vmem(lines, 2, 2, 8, 4 * quarter),
                vmem(lines, 2, 2, 8, 3 * quarter),
                vmem(lines, 2, 2, 8, 2 * quarter),
                vmem(lines, 2, 2, 8, quarter),
                vmem(lines, 2, 8, quarter),
                vmem(lines, 8, quarter),
                vmem(*norm_in.shape),
                vmem(2, 2, count, 1, shard),
                vmem(2, 2, count, 1, shard),
                vmem(2, 2, count, 1, shard),
                vmem(2, count, 1, shard),
                vmem(count, 1, shard),
                vmem(count, 1, shard),
                vmem(count, 1, shard),
                vmem(8, LANES),
                vmem(8, LANES),
                vmem(9, 8, LANES),
                dma, dma((rounds,)), dma((SLOTS,)),
                dma((2,)), dma((2, rounds)), dma((2,)), dma((2, rounds)),
                dma, dma((rounds,)), dma, dma((rounds,)), dma,
                dma, dma,
                dma((lines,)), dma((9,)), dma((9, lines)),
                dma, dma((6,)), dma((6,)), dma, dma,
            ],
            compiler_params=pltpu.CompilerParams(collective_id=0, has_side_effects=True, vmem_limit_bytes=VMEM_MIB << 20),
            name="reduce_gradients",
        )(emb_in, mat_in, norm_in)
        block = pl.BlockSpec((ADAM_ROWS, width), lambda i: (i, 0))
        whole_mat = pl.BlockSpec((mat_rows, width), lambda i: (0, 0))
        whole_norm = pl.BlockSpec((count, shard), lambda i: (0, 0))
        specs = [block] * 4 + [whole_mat] * 4 + [whole_norm] * 4
        shapes = []
        for like in (emb_param, mat_param, norm_param):
            shapes += [jax.ShapeDtypeStruct(like.shape, F32)] * 3 + [jax.ShapeDtypeStruct(like.shape, jnp.bfloat16)]
        return pl.pallas_call(
            adam_kernel,
            grid=(emb_rows // ADAM_ROWS,),
            out_shape=tuple(shapes),
            in_specs=[pl.BlockSpec((8, LANES), lambda i: (0, 0))] + specs,
            out_specs=tuple(specs),
            compiler_params=pltpu.CompilerParams(vmem_limit_bytes=24 << 20),
            name="adam",
        )(scale, emb_mean, emb_param, emb_mom, emb_var, mat_mean, mat_param, mat_mom, mat_var,
          norm_mean, norm_param, norm_mom, norm_var)

    grad_spec = P("dp", "fsdp", None, None)
    row_spec = P("fsdp", None)
    col_spec = P(None, "fsdp")
    in_list = (grad_spec, grad_spec, grad_spec, row_spec, row_spec, row_spec, row_spec, row_spec, row_spec, col_spec, col_spec, col_spec)
    out_list = (row_spec, row_spec, row_spec, row_spec, row_spec, row_spec, row_spec, row_spec, col_spec, col_spec, col_spec, col_spec)
    return jax.shard_map(local_step, mesh=mesh, in_specs=in_list, out_specs=out_list, check_vma=False)
```

```python
import functools

import jax
import jax.numpy as jnp
from jax import lax
from jax.experimental import pallas as pl
from jax.experimental.pallas import tpu as pltpu
from jax.sharding import PartitionSpec as P

LEARN_RATE = 0.003
BETA_ONE = 0.9
BETA_TWO = 0.95
ADAM_EPS = 1e-8
WEIGHT_DECAY = 0.1
CLIP_NORM = 1.0
ADAM_STEP = 10

MESH = pl.DeviceIdType.MESH
F32 = jnp.float32
LANES = 128
SPLIT = 2
AHEAD = 2
SLOTS = 4
STATE_ROUND = 16
CORE_AHEAD = 4
LAG_ONE, LAG_TWO, LAG_SIDE, LAG_MID, LAG_BACK = 2, 4, 6, 8, 10
NORM_START, NORM_STEP = 8, 6
LINE_BLOCKS = 4
LINE_SPLIT = 3
LINE_RATE, LINE_STEP = 4, 2
ADAM_ROWS, ADAM_COLS = 16, 512
VMEM_KIB, ADAM_MIB = 45568, 20


def reduce_kernel(inv_count, emb_ref, mat_ref, norm_ref, *refs):
    emb_state, mat_state, state_out = refs[0:3], refs[3:6], refs[9:12]
    mean_out, norm_out, scale_out = refs[6:9]
    (acc, own, one, two, zmid, lown, lside, lmid, lback, lone, ltwo,
     norm_all, nsend, nown, nacc, none, ntwo, nzin, nzmid, sq_main, sq_line, sq_all,
     core_send, core_recv, own_sem, one_send, one_recv, two_send, two_recv,
     side_send, side_recv, mid_send, mid_recv, back_send,
     lown_sem, line_send, line_recv, norm_sem, nsend_sem, nrecv_sem, sq_send, sq_recv, scale_send, scale_recv, state_sem) = refs[12:]
    z = lax.axis_index("dp")
    f = lax.axis_index("fsdp")
    y, x, c = f // 4, (f // 2) % 2, f % 2
    width = acc.shape[3]
    half = width // 2
    cols = half // SPLIT
    emb_blocks = emb_ref.shape[3] // 8
    rounds = one.shape[2] // 8 * SPLIT
    emb_rounds = (emb_blocks - LINE_BLOCKS) * SPLIT
    lines = lside.shape[0]
    lwidth = width // LINE_SPLIT
    quarter = lwidth // 4
    is_end = (z == 0) | (z == 3)
    is_mid = (z == 1) | (z == 2)
    high = z // 2
    side = z + 1 - 2 * (z % 2)
    core_peer = (z, y * 4 + x * 2 + 1 - c)
    x_peer = (z, y * 4 + (1 - x) * 2 + c)
    y_peer = (z, (1 - y) * 4 + x * 2 + c)
    side_peer = (side, f)
    mid_peer = (lax.rem(3 - z, 4), f)

    def remote(src, dst, send_sem, recv_sem, peer):
        return pltpu.make_async_remote_copy(src, dst, send_sem, recv_sem, device_id=peer, device_id_type=MESH)

    def take(ref, sem):
        pltpu.make_async_copy(ref, ref, sem).wait()

    def piece(q):
        block, sub = lax.div(q, SPLIT), lax.rem(q, SPLIT) * cols
        rows = pl.ds(pl.multiple_of((block + LINE_BLOCKS) * 8, 8), 8)
        inner = pl.ds(pl.multiple_of(block * 8, 8), 8)
        wide = [pl.ds(pl.multiple_of(sub + h * half, LANES), cols) for h in range(2)]
        return rows, inner, wide, pl.ds(pl.multiple_of(sub, LANES), cols)

    def mat_rows(q):
        return pl.ds(pl.multiple_of((lax.div(q, SPLIT) + LINE_BLOCKS - emb_blocks) * 8, 8), 8)

    def from_emb_or_mat(q, do):
        rows, _, wide, _ = piece(q)

        @pl.when(q < emb_rounds)
        def _():
            for h in range(2):
                do(emb_ref, rows, h, wide[h])

        @pl.when(q >= emb_rounds)
        def _():
            for h in range(2):
                do(mat_ref, mat_rows(q), h, wide[h])

    def load_own(q):
        slot = lax.rem(q, SLOTS)
        from_emb_or_mat(q, lambda ref, rows, h, cs: pltpu.make_async_copy(
            ref.at[:, :, c, rows, cs], own.at[slot, h], own_sem.at[slot]).start())

    def send_core(q):
        rb = piece(q)[0]
        from_emb_or_mat(q, lambda ref, rows, h, cs: remote(
            ref.at[:, :, 1 - c, rows, cs], acc.at[:, :, rb, cs], core_send, core_recv.at[q], core_peer).start())

    def line_at(i, start=0, size=4):
        rows = pl.ds(pl.multiple_of(lax.div(i, LINE_SPLIT) * 8, 8), 8)
        return rows, pl.ds(pl.multiple_of(lax.rem(i, LINE_SPLIT) * lwidth + start * quarter, LANES), size * quarter)

    def load_line(i):
        rows, cs = line_at(i)
        slot = lax.rem(i, SLOTS)
        return pltpu.make_async_copy(emb_ref.at[:, :, c, rows, cs], lown.at[slot], lown_sem.at[slot])

    def line_core(i):
        rows, cs = line_at(i)
        return remote(emb_ref.at[:, :, 1 - c, rows, cs], acc.at[:, :, rows, cs], line_send.at[0], line_recv.at[0, i], core_peer)

    norm_load = pltpu.make_async_copy(norm_ref, norm_all, norm_sem)
    norm_load.start()
    for q in range(AHEAD):
        load_own(jnp.int32(q))
    load_line(jnp.int32(0)).start()

    barrier = pltpu.get_barrier_semaphore()
    pl.semaphore_signal(barrier, inc=1, device_id=side_peer, device_id_type=MESH)

    @pl.when(is_mid)
    def _():
        for step in range(1, 8):
            pl.semaphore_signal(barrier, inc=1, device_id=(z, lax.rem(f + step, 8)), device_id_type=MESH)
        pl.semaphore_signal(barrier, inc=1, device_id=mid_peer, device_id_type=MESH)
        pl.semaphore_wait(barrier, 9)

    @pl.when(is_end)
    def _():
        for peer in (core_peer, x_peer, y_peer):
            pl.semaphore_signal(barrier, inc=1, device_id=peer, device_id_type=MESH)
        pl.semaphore_wait(barrier, 4)

    for q in range(CORE_AHEAD):
        send_core(jnp.int32(q))
        if q == 0:
            line_core(jnp.int32(0)).start()

    sq_main[...] = jnp.zeros_like(sq_main)
    sq_line[...] = jnp.zeros_like(sq_line)

    def one_copy(q, h):
        rb, inner, wide, cs = piece(q)
        src = acc.at[:, 1 - x, rb, wide[0]] if h == 0 else acc.at[1 - y, :, rb, wide[1]]
        return remote(src, one.at[h, :, inner, cs], one_send.at[h], one_recv.at[h, q], (x_peer, y_peer)[h])

    def two_copy(q, h):
        rb, inner, wide, cs = piece(q)
        src = acc.at[1 - y, x, rb, wide[0]] if h == 0 else acc.at[y, 1 - x, rb, wide[1]]
        return remote(src, two.at[h, inner, cs], two_send.at[h], two_recv.at[h, q], (y_peer, x_peer)[h])

    def side_copy(q, h):
        rb, _, wide, _ = piece(q)
        return remote(acc.at[y, x, rb, wide[h]], mean_out.at[rb, wide[h]], side_send, side_recv.at[h, q], side_peer)

    def mid_copy(q, h):
        rb, inner, wide, _ = piece(q)
        return remote(acc.at[y, x, rb, wide[h]], zmid.at[inner, wide[h]], mid_send, mid_recv.at[h, q], mid_peer)

    def back_copy(q, h):
        rb, _, wide, _ = piece(q)
        return remote(mean_out.at[rb, wide[h]], mean_out.at[rb, wide[h]], back_send, side_recv.at[h, q], side_peer)

    def add_squares(part_ref, total):
        sq = total * total
        part = part_ref[...]
        for j in range(total.shape[1] // LANES):
            part = part + sq[:, j * LANES:(j + 1) * LANES]
        part_ref[...] = part

    def line_side(i):
        rows, cs = line_at(i, 1 - high, 3)
        return remote(acc.at[:, :, rows, cs], lside.at[i], line_send.at[1], line_recv.at[1, i], side_peer)

    def line_mid(i):
        rows, cs = line_at(i, 2 - 2 * high, 2)
        return remote(acc.at[:, :, rows, cs], lmid.at[i], line_send.at[2], line_recv.at[2, i], mid_peer)

    def line_back(i):
        rows, cs = line_at(i, 3 * high, 1)
        return remote(acc.at[:, :, rows, cs], lback.at[i], line_send.at[3], line_recv.at[3, i], side_peer)

    def line_one(i, h):
        rows, cs = line_at(i, z, 1)
        src = acc.at[:, 1 - x, rows, cs] if h == 0 else acc.at[1 - y, :, rows, cs]
        return remote(src, lone.at[i], line_send.at[4], line_recv.at[4, i], (x_peer, y_peer)[h])

    def line_two(i, h):
        rows, cs = line_at(i, z, 1)
        src = acc.at[1 - y, x, rows, cs] if h == 0 else acc.at[y, 1 - x, rows, cs]
        return remote(src, ltwo.at[i], line_send.at[5], line_recv.at[5, i], (y_peer, x_peer)[h])

    def gather_side(i):
        rows, cs = line_at(i, 3 * high, 1)
        return remote(mean_out.at[rows, cs], mean_out.at[rows, cs], line_send.at[6], line_recv.at[6, i], side_peer)

    def gather_mid(i):
        rows, cs = line_at(i, 2 * high, 2)
        return remote(mean_out.at[rows, cs], mean_out.at[rows, cs], line_send.at[7], line_recv.at[7, i], mid_peer)

    def gather_back(i):
        rows, cs = line_at(i, 1 - high, 3)
        return remote(mean_out.at[rows, cs], mean_out.at[rows, cs], line_send.at[8], line_recv.at[8, i], side_peer)

    def either_way(i, do):
        @pl.when(lax.rem(i, 2) == 0)
        def _():
            do(0)

        @pl.when(lax.rem(i, 2) == 1)
        def _():
            do(1)

    def line_stage_0(i):
        rows, cs = line_at(i)
        load_line(i).wait()
        slot = lax.rem(i, SLOTS)
        take(lown.at[slot], line_recv.at[0, i])
        acc[:, :, rows, cs] = acc[:, :, rows, cs] + lown[slot]

        @pl.when(is_end)
        def _():
            line_side(i).start()

    def line_stage_1(i):
        @pl.when(is_mid)
        def _():
            rows, cs = line_at(i, 1 - high, 3)
            take(lside.at[i], line_recv.at[1, i])
            acc[:, :, rows, cs] = acc[:, :, rows, cs] + lside[i]
            line_mid(i).start()

    def line_stage_2(i):
        @pl.when(is_mid)
        def _():
            rows, cs = line_at(i, 2 * high, 2)
            take(lmid.at[i], line_recv.at[2, i])
            acc[:, :, rows, cs] = acc[:, :, rows, cs] + lmid[i]
            line_back(i).start()

    def line_stage_3(i):
        @pl.when(is_end)
        def _():
            rows, cs = line_at(i, 3 * high, 1)
            take(lback.at[i], line_recv.at[3, i])
            acc[:, :, rows, cs] = acc[:, :, rows, cs] + lback[i]

        either_way(i, lambda h: line_one(i, h).start())

    def line_stage_4(i):
        rows, cs = line_at(i, z, 1)
        take(lone.at[i], line_recv.at[4, i])

        def add(h):
            if h == 0:
                acc[:, x, rows, cs] = acc[:, x, rows, cs] + lone[i]
            else:
                acc[y, :, rows, cs] = acc[y, :, rows, cs] + lone[i]
            line_two(i, h).start()

        either_way(i, add)

    def line_stage_5(i):
        rows, cs = line_at(i, z, 1)
        take(ltwo.at[i], line_recv.at[5, i])
        mean_out[rows, cs] = (acc[y, x, rows, cs] + ltwo[i]) * inv_count

        @pl.when(is_end)
        def _():
            gather_side(i).start()

    def line_stage_6(i):
        @pl.when(is_mid)
        def _():
            take(ltwo.at[i], line_recv.at[6, i])
            gather_mid(i).start()

    def line_stage_7(i):
        @pl.when(is_mid)
        def _():
            take(lone.at[i], line_recv.at[7, i])
            gather_back(i).start()
            rows, cs = line_at(i)
            add_squares(sq_line, mean_out[rows, cs])

    def line_stage_8(i):
        @pl.when(is_end)
        def _():
            take(lside.at[i, 0, 0], line_recv.at[8, i])

    line_stages = (line_stage_0, line_stage_1, line_stage_2, line_stage_3, line_stage_4, line_stage_5, line_stage_6,
                   line_stage_7, line_stage_8)

    norm_core = remote(nsend, nacc, nsend_sem.at[0], nrecv_sem.at[0], core_peer)
    norm_one = remote(nacc.at[:, 1 - x], none, nsend_sem.at[1], nrecv_sem.at[1], x_peer)
    norm_two = remote(nacc.at[1 - y, x], ntwo, nsend_sem.at[2], nrecv_sem.at[2], y_peer)
    norm_side = remote(nacc.at[y, x], nzin, nsend_sem.at[3], nrecv_sem.at[3], side_peer)
    norm_mid = remote(nacc.at[y, x], nzmid, nsend_sem.at[4], nrecv_sem.at[4], mid_peer)
    norm_back = remote(nzin, nzin, nsend_sem.at[5], nrecv_sem.at[3], side_peer)
    def state_parts(j):
        split = emb_state[j].shape[0]
        return ((emb_state[j], state_out[j].at[pl.ds(0, split)]),
                (mat_state[j], state_out[j].at[pl.ds(split, mat_state[j].shape[0])]))

    def body(t, carry):
        @pl.when(t + CORE_AHEAD < rounds)
        def _():
            send_core(t + CORE_AHEAD)

        @pl.when(t + AHEAD < rounds)
        def _():
            load_own(t + AHEAD)

        early = t + CORE_AHEAD

        @pl.when((lax.rem(early, LINE_RATE) == 0) & (early < lines * LINE_RATE))
        def _():
            line_core(lax.div(early, LINE_RATE)).start()
            load_line(lax.div(early, LINE_RATE)).start()

        @pl.when(t < rounds)
        def _():
            rb, _, wide, _ = piece(t)
            slot = lax.rem(t, SLOTS)
            take(own.at[slot], own_sem.at[slot])
            take(own.at[slot], core_recv.at[t])
            for h in range(2):
                acc[:, :, rb, wide[h]] = acc[:, :, rb, wide[h]] + own[slot, h]
                one_copy(t, h).start()

        q1 = t - LAG_ONE

        @pl.when((q1 >= 0) & (q1 < rounds))
        def _():
            rb, inner, wide, cs = piece(q1)
            one_copy(q1, 0).wait_recv()
            acc[:, x, rb, wide[0]] = acc[:, x, rb, wide[0]] + one[0, :, inner, cs]
            two_copy(q1, 0).start()
            one_copy(q1, 1).wait_recv()
            acc[y, :, rb, wide[1]] = acc[y, :, rb, wide[1]] + one[1, :, inner, cs]
            two_copy(q1, 1).start()

        q2 = t - LAG_TWO

        @pl.when((q2 >= 0) & (q2 < rounds))
        def _():
            rb, inner, wide, cs = piece(q2)
            for h in range(2):
                two_copy(q2, h).wait_recv()
                acc[y, x, rb, wide[h]] = acc[y, x, rb, wide[h]] + two[h, inner, cs]

                @pl.when(is_end)
                def _(h=h):
                    side_copy(q2, h).start()

        q3 = t - LAG_SIDE

        @pl.when(is_mid & (q3 >= 0) & (q3 < rounds))
        def _():
            rb, _, wide, _ = piece(q3)
            for h in range(2):
                side_copy(q3, h).wait_recv()
                acc[y, x, rb, wide[h]] = acc[y, x, rb, wide[h]] + mean_out[rb, wide[h]]
                mid_copy(q3, h).start()

        q4 = t - LAG_MID

        @pl.when(is_mid & (q4 >= 0) & (q4 < rounds))
        def _():
            rb, inner, wide, _ = piece(q4)
            for h in range(2):
                mid_copy(q4, h).wait_recv()
                total = (acc[y, x, rb, wide[h]] + zmid[inner, wide[h]]) * inv_count
                mean_out[rb, wide[h]] = total
                back_copy(q4, h).start()
                add_squares(sq_main, total)

        q5 = t - LAG_BACK

        @pl.when(is_end & (q5 >= 0) & (q5 < rounds))
        def _():
            for h in range(2):
                back_copy(q5, h).wait_recv()

        for k, stage in enumerate(line_stages):
            late = t - k * LINE_STEP

            @pl.when((late >= 0) & (late < lines * LINE_RATE) & (lax.rem(late, LINE_RATE) == 0))
            def _(late=late, stage=stage):
                stage(lax.div(late, LINE_RATE))

        @pl.when(t == STATE_ROUND)
        def _():
            for j in range(3):
                for src, dst in state_parts(j):
                    pltpu.make_async_copy(src, dst, state_sem.at[j]).start()

        @pl.when(t == NORM_START - NORM_STEP)
        def _():
            norm_load.wait()
            shard = nacc.shape[4]
            for yy in range(2):
                for xx in range(2):
                    at = (4 * yy + 2 * xx) * shard
                    first = norm_all[:, :, at:at + shard]
                    second = norm_all[:, :, at + shard:at + 2 * shard]
                    nsend[yy, xx] = jnp.where(c == 0, second, first)
                    nown[yy, xx] = jnp.where(c == 0, first, second)
            norm_core.start()

        @pl.when(t == NORM_START)
        def _():
            norm_core.wait_recv()
            nacc[...] = nacc[...] + nown[...]
            norm_one.start()

        @pl.when(t == NORM_START + NORM_STEP)
        def _():
            norm_one.wait_recv()
            nacc[:, x] = nacc[:, x] + none[...]
            norm_two.start()

        @pl.when(t == NORM_START + 2 * NORM_STEP)
        def _():
            norm_two.wait_recv()
            nacc[y, x] = nacc[y, x] + ntwo[...]

            @pl.when(is_end)
            def _():
                norm_side.start()

        @pl.when(is_mid & (t == NORM_START + 3 * NORM_STEP))
        def _():
            norm_side.wait_recv()
            nacc[y, x] = nacc[y, x] + nzin[...]
            norm_mid.start()

        @pl.when(is_mid & (t == NORM_START + 4 * NORM_STEP))
        def _():
            norm_mid.wait_recv()
            nzin[...] = (nacc[y, x] + nzmid[...]) * inv_count
            norm_back.start()

        @pl.when(is_end & (t == NORM_START + 5 * NORM_STEP))
        def _():
            norm_back.wait_recv()

        @pl.when(t == NORM_START + 6 * NORM_STEP)
        def _():
            for j in range(norm_out.shape[0]):
                norm_out[j:j + 1, :] = nzin[j]
            norm_total = nzin[...]
            norm_sq = jnp.sum(norm_total * norm_total)
            corner = [lax.broadcasted_iota(jnp.int32, sq_line.shape, d) == 0 for d in range(2)]
            sq_norm = jnp.where(corner[0] & corner[1], norm_sq, 0.0)
            sq_all[0] = sq_norm

        return carry

    lax.fori_loop(0, rounds + LAG_BACK, body, 0)

    for j in range(3):
        take(state_out[j], state_sem.at[j])
    scale_copy = remote(scale_out, scale_out, scale_send, scale_recv, side_peer)

    @pl.when(is_mid)
    def _():
        sq_main[...] = sq_main[...] + sq_line[...] + sq_all[0]
        for step in range(1, 8):
            remote(sq_main, sq_all.at[1 + f], sq_send, sq_recv, (z, lax.rem(f + step, 8))).start()
        sq_all[1 + f] = sq_main[...]
        seven = sq_all.at[pl.ds(0, 7)]
        take(seven, sq_recv)
        square = sq_all[1]
        for j in range(2, 9):
            square = square + sq_all[j]
        scale_out[...] = jnp.minimum(1.0, CLIP_NORM / jnp.sqrt(jnp.broadcast_to(jnp.sum(square), square.shape)))
        scale_copy.start()
        take(seven, sq_send)

    @pl.when(is_end)
    def _():
        scale_copy.wait_recv()

    take(acc.at[:, :, pl.ds(0, one.shape[2])], core_send)
    for h in range(2):
        take(one.at[h], one_send.at[h])
        take(two.at[h], two_send.at[h])
    take(acc.at[:, :, pl.ds(0, 8 * LINE_BLOCKS)], line_send.at[0])
    take(lone, line_send.at[4])
    take(ltwo, line_send.at[5])
    norm_core.wait_send()
    norm_one.wait_send()
    norm_two.wait_send()

    @pl.when(is_end)
    def _():
        take(zmid, side_send)
        take(lside, line_send.at[1])
        take(ltwo, line_send.at[6])
        norm_side.wait_send()

    @pl.when(is_mid)
    def _():
        take(zmid, mid_send)
        take(zmid, back_send)
        take(lmid, line_send.at[2])
        take(lback, line_send.at[3])
        take(lone, line_send.at[7])
        take(lside.at[:, 0, 0], line_send.at[8])
        norm_mid.wait_send()
        norm_back.wait_send()
        scale_copy.wait_send()


def adam_kernel(scale_ref, mean_ref, norm_ref, *refs):
    ins, outs, news, sems = refs[:6], refs[6:18], refs[18:30], refs[30]
    clip = scale_ref[0:1, 0:1]
    rate = LEARN_RATE / (1.0 - BETA_ONE ** ADAM_STEP)
    bias_two = 1.0 / (1.0 - BETA_TWO ** ADAM_STEP)
    emb_rows = outs[0].shape[0]

    def update(group, grad_ref, states, source, start, rows, decay_rate):
        width = grad_ref.shape[1]
        cols = ADAM_COLS if width % ADAM_COLS == 0 else width
        at, here = pl.ds(start, rows), pl.ds(source + start, rows)
        for left in range(0, width, cols):
            cs = pl.ds(left, cols)
            grad = grad_ref[here, cs] * clip
            param, mom, var = (ref[here, cs] for ref in states)
            new_mom = BETA_ONE * mom + (1.0 - BETA_ONE) * grad
            new_var = BETA_TWO * var + (1.0 - BETA_TWO) * grad * grad
            move = rate * new_mom / (jnp.sqrt(new_var * bias_two) + ADAM_EPS)
            new_param = (1.0 - LEARN_RATE * decay_rate) * param - move
            for ref, value in zip(news[4 * group:4 * group + 4], (new_param, new_mom, new_var, new_param)):
                ref[at, cs] = value.astype(ref.dtype)
        for k in range(4 * group, 4 * group + 4):
            pltpu.make_async_copy(news[k].at[at], outs[k].at[at], sems.at[k]).start()

    update(2, norm_ref, ins[3:], 0, 0, norm_ref.shape[0], 0.0)
    update(1, mean_ref, ins[:3], emb_rows, 0, outs[4].shape[0], WEIGHT_DECAY)

    def some_rows(r, carry):
        update(0, mean_ref, ins[:3], 0, pl.multiple_of(r * ADAM_ROWS, ADAM_ROWS), ADAM_ROWS, WEIGHT_DECAY)
        return carry

    lax.fori_loop(0, emb_rows // ADAM_ROWS, some_rows, 0)
    for k in range(12):
        pltpu.make_async_copy(outs[k], outs[k], sems.at[k]).wait()


def solution(mesh):
    dev_count = mesh.shape["dp"] * mesh.shape["fsdp"]

    def local_step(emb_grad, mat_grad, norm_grad, emb_param, emb_mom, emb_var, mat_param, mat_mom, mat_var, norm_param, norm_mom, norm_var):
        width = emb_grad.shape[3]
        emb_rows, mat_rows = emb_param.shape[0], mat_param.shape[0]
        count, shard = norm_param.shape
        emb_in = emb_grad.reshape(2, 2, 2, emb_rows, width)
        mat_in = mat_grad.reshape(2, 2, 2, mat_rows, width)
        norm_in = norm_grad.reshape(count, 1, norm_grad.shape[3])
        rows = emb_rows + mat_rows
        main_rows = rows - 8 * LINE_BLOCKS
        rounds = main_rows // 8 * SPLIT
        half = width // 2
        lines = LINE_BLOCKS * LINE_SPLIT
        quarter = width // LINE_SPLIT // 4
        any_spec = pl.BlockSpec(memory_space=pl.ANY)
        vmem_spec = pl.BlockSpec(memory_space=pltpu.VMEM)
        dma = pltpu.SemaphoreType.DMA
        vmem = lambda *shape: pltpu.VMEM(shape, F32)
        mean, norm_mean, scale, param, mom, var = pl.pallas_call(
            functools.partial(reduce_kernel, 1.0 / dev_count),
            out_shape=(
                vmem(rows, width),
                vmem(count, shard),
                vmem(8, LANES),
            ) + (vmem(rows, width),) * 3,
            in_specs=[any_spec] * 9,
            out_specs=(vmem_spec,) * 6,
            scratch_shapes=[
                vmem(2, 2, rows, width),
                vmem(SLOTS, 2, 2, 2, 8, half // SPLIT),
                vmem(2, 2, main_rows, half),
                vmem(2, main_rows, half),
                vmem(main_rows, width),
                vmem(SLOTS, 2, 2, 8, 4 * quarter),
                vmem(lines, 2, 2, 8, 3 * quarter),
                vmem(lines, 2, 2, 8, 2 * quarter),
                vmem(lines, 2, 2, 8, quarter),
                vmem(lines, 2, 8, quarter),
                vmem(lines, 8, quarter),
                vmem(*norm_in.shape),
                vmem(2, 2, count, 1, shard),
                vmem(2, 2, count, 1, shard),
                vmem(2, 2, count, 1, shard),
                vmem(2, count, 1, shard),
                vmem(count, 1, shard),
                vmem(count, 1, shard),
                vmem(count, 1, shard),
                vmem(8, LANES),
                vmem(8, LANES),
                vmem(9, 8, LANES),
                dma, dma((rounds,)), dma((SLOTS,)),
                dma((2,)), dma((2, rounds)), dma((2,)), dma((2, rounds)),
                dma, dma((2, rounds)), dma, dma((2, rounds)), dma,
                dma((SLOTS,)), dma((9,)), dma((9, lines)),
                dma, dma((6,)), dma((6,)), dma, dma, dma, dma, dma((3,)),
            ],
            compiler_params=pltpu.CompilerParams(collective_id=0, has_side_effects=True, vmem_limit_bytes=VMEM_KIB << 10),
            name="reduce_gradients",
        )(*(pltpu.with_memory_space_constraint(a, pltpu.HBM) for a in (
            emb_in, mat_in, norm_in, emb_param, emb_mom, emb_var, mat_param, mat_mom, mat_var)))
        shapes = []
        for like in (emb_param, mat_param, norm_param):
            shapes += [jax.ShapeDtypeStruct(like.shape, F32)] * 3 + [jax.ShapeDtypeStruct(like.shape, jnp.bfloat16)]
        return pl.pallas_call(
            adam_kernel,
            out_shape=tuple(shapes),
            in_specs=[vmem_spec] * 9,
            out_specs=(any_spec,) * 12,
            scratch_shapes=[pltpu.VMEM(like.shape, like.dtype) for like in shapes] + [dma((12,))],
            compiler_params=pltpu.CompilerParams(vmem_limit_bytes=ADAM_MIB << 20),
            name="adam",
        )(scale, mean, norm_mean, param, mom, var, norm_param, norm_mom, norm_var)

    grad_spec = P("dp", "fsdp", None, None)
    row_spec = P("fsdp", None)
    col_spec = P(None, "fsdp")
    in_list = (grad_spec, grad_spec, grad_spec, row_spec, row_spec, row_spec, row_spec, row_spec, row_spec, col_spec, col_spec, col_spec)
    out_list = (row_spec, row_spec, row_spec, row_spec, row_spec, row_spec, row_spec, row_spec, col_spec, col_spec, col_spec, col_spec)
    return jax.shard_map(local_step, mesh=mesh, in_specs=in_list, out_specs=out_list, check_vma=False)
```

```python
import functools

import jax
import jax.numpy as jnp
from jax import lax
from jax.experimental import pallas as pl
from jax.experimental.pallas import tpu as pltpu
from jax.sharding import PartitionSpec as P

LEARN_RATE = 0.003
BETA_ONE = 0.9
BETA_TWO = 0.95
ADAM_EPS = 1e-8
WEIGHT_DECAY = 0.1
CLIP_NORM = 1.0
ADAM_STEP = 10

MESH = pl.DeviceIdType.MESH
F32 = jnp.float32
LANES = 128
SPLIT = 2
AHEAD = 2
SLOTS = 4
CORE_RING, RING, LINE_RING = 12, 8, 4
STATE_ROUND = 16
CORE_AHEAD = 4
LAG_ONE, LAG_TWO, LAG_SIDE, LAG_MID, LAG_BACK = 2, 4, 6, 8, 10
NORM_START, NORM_STEP = 8, 6
LINE_BLOCKS = 4
LINE_SPLIT = 3
LINE_RATE, LINE_STEP = 4, 2
ADAM_ROWS, ADAM_COLS = 16, 512
VMEM_KIB, ADAM_MIB = 45568, 20


def reduce_kernel(inv_count, emb_ref, mat_ref, norm_ref, *refs):
    emb_state, mat_state, state_out = refs[0:3], refs[3:6], refs[9:12]
    mean_out, norm_out, scale_out = refs[6:9]
    (acc, own, one, two, zmid, lown, lside, lmid, lback, lone, ltwo,
     norm_all, nsend, nown, nacc, none, ntwo, nzin, nzmid, sq_main, sq_line, sq_all,
     core_send, core_recv, own_sem, one_send, one_recv, two_send, two_recv,
     side_send, side_recv, mid_send, mid_recv, back_send,
     lown_sem, line_send, line_recv, norm_sem, nsend_sem, nrecv_sem, sq_send, sq_recv, scale_send, scale_recv, state_sem) = refs[12:]
    z = lax.axis_index("dp")
    f = lax.axis_index("fsdp")
    y, x, c = f // 4, (f // 2) % 2, f % 2
    width = acc.shape[3]
    half = width // 2
    cols = half // SPLIT
    emb_blocks = emb_ref.shape[3] // 8
    rounds = one.shape[2] // 8 * SPLIT
    emb_rounds = (emb_blocks - LINE_BLOCKS) * SPLIT
    lines = lside.shape[0]
    lwidth = width // LINE_SPLIT
    quarter = lwidth // 4
    is_end = (z == 0) | (z == 3)
    is_mid = (z == 1) | (z == 2)
    high = z // 2
    side = z + 1 - 2 * (z % 2)
    core_peer = (z, y * 4 + x * 2 + 1 - c)
    x_peer = (z, y * 4 + (1 - x) * 2 + c)
    y_peer = (z, (1 - y) * 4 + x * 2 + c)
    side_peer = (side, f)
    mid_peer = (lax.rem(3 - z, 4), f)

    def remote(src, dst, send_sem, recv_sem, peer):
        return pltpu.make_async_remote_copy(src, dst, send_sem, recv_sem, device_id=peer, device_id_type=MESH)

    def take(ref, sem):
        pltpu.make_async_copy(ref, ref, sem).wait()

    def ring(q):
        return lax.rem(q, RING)

    def line_ring(i):
        return lax.rem(i, LINE_RING)

    def piece(q):
        block, sub = lax.div(q, SPLIT), lax.rem(q, SPLIT) * cols
        rows = pl.ds(pl.multiple_of((block + LINE_BLOCKS) * 8, 8), 8)
        inner = pl.ds(pl.multiple_of(block * 8, 8), 8)
        wide = [pl.ds(pl.multiple_of(sub + h * half, LANES), cols) for h in range(2)]
        return rows, inner, wide, pl.ds(pl.multiple_of(sub, LANES), cols)

    def mat_rows(q):
        return pl.ds(pl.multiple_of((lax.div(q, SPLIT) + LINE_BLOCKS - emb_blocks) * 8, 8), 8)

    def from_emb_or_mat(q, do):
        rows, _, wide, _ = piece(q)

        @pl.when(q < emb_rounds)
        def _():
            for h in range(2):
                do(emb_ref, rows, h, wide[h])

        @pl.when(q >= emb_rounds)
        def _():
            for h in range(2):
                do(mat_ref, mat_rows(q), h, wide[h])

    def load_own(q):
        slot = lax.rem(q, SLOTS)
        from_emb_or_mat(q, lambda ref, rows, h, cs: pltpu.make_async_copy(
            ref.at[:, :, c, rows, cs], own.at[slot, h], own_sem.at[slot]).start())

    def send_core(q):
        rb = piece(q)[0]
        from_emb_or_mat(q, lambda ref, rows, h, cs: remote(
            ref.at[:, :, 1 - c, rows, cs], acc.at[:, :, rb, cs], core_send, core_recv.at[lax.rem(q, CORE_RING)], core_peer).start())

    def line_at(i, start=0, size=4):
        rows = pl.ds(pl.multiple_of(lax.div(i, LINE_SPLIT) * 8, 8), 8)
        return rows, pl.ds(pl.multiple_of(lax.rem(i, LINE_SPLIT) * lwidth + start * quarter, LANES), size * quarter)

    def load_line(i):
        rows, cs = line_at(i)
        slot = lax.rem(i, SLOTS)
        return pltpu.make_async_copy(emb_ref.at[:, :, c, rows, cs], lown.at[slot], lown_sem.at[slot])

    def line_core(i):
        rows, cs = line_at(i)
        return remote(emb_ref.at[:, :, 1 - c, rows, cs], acc.at[:, :, rows, cs], line_send.at[0], line_recv.at[0, line_ring(i)], core_peer)

    norm_load = pltpu.make_async_copy(norm_ref, norm_all, norm_sem)
    norm_load.start()
    for q in range(AHEAD):
        load_own(jnp.int32(q))
    load_line(jnp.int32(0)).start()

    barrier = pltpu.get_barrier_semaphore()
    pl.semaphore_signal(barrier, inc=1, device_id=side_peer, device_id_type=MESH)

    @pl.when(is_mid)
    def _():
        for step in range(1, 8):
            pl.semaphore_signal(barrier, inc=1, device_id=(z, lax.rem(f + step, 8)), device_id_type=MESH)
        pl.semaphore_signal(barrier, inc=1, device_id=mid_peer, device_id_type=MESH)
        pl.semaphore_wait(barrier, 9)

    @pl.when(is_end)
    def _():
        for peer in (core_peer, x_peer, y_peer):
            pl.semaphore_signal(barrier, inc=1, device_id=peer, device_id_type=MESH)
        pl.semaphore_wait(barrier, 4)

    for q in range(CORE_AHEAD):
        send_core(jnp.int32(q))
        if q == 0:
            line_core(jnp.int32(0)).start()

    sq_main[...] = jnp.zeros_like(sq_main)
    sq_line[...] = jnp.zeros_like(sq_line)

    def one_copy(q, h):
        rb, inner, wide, cs = piece(q)
        src = acc.at[:, 1 - x, rb, wide[0]] if h == 0 else acc.at[1 - y, :, rb, wide[1]]
        return remote(src, one.at[h, :, inner, cs], one_send.at[h], one_recv.at[h, ring(q)], (x_peer, y_peer)[h])

    def two_copy(q, h):
        rb, inner, wide, cs = piece(q)
        src = acc.at[1 - y, x, rb, wide[0]] if h == 0 else acc.at[y, 1 - x, rb, wide[1]]
        return remote(src, two.at[h, inner, cs], two_send.at[h], two_recv.at[h, ring(q)], (y_peer, x_peer)[h])

    def side_copy(q, h):
        rb, _, wide, _ = piece(q)
        return remote(acc.at[y, x, rb, wide[h]], mean_out.at[rb, wide[h]], side_send, side_recv.at[h, ring(q)], side_peer)

    def mid_copy(q, h):
        rb, inner, wide, _ = piece(q)
        return remote(acc.at[y, x, rb, wide[h]], zmid.at[inner, wide[h]], mid_send, mid_recv.at[h, ring(q)], mid_peer)

    def back_copy(q, h):
        rb, _, wide, _ = piece(q)
        return remote(mean_out.at[rb, wide[h]], mean_out.at[rb, wide[h]], back_send, side_recv.at[h, ring(q)], side_peer)

    def add_squares(part_ref, total):
        sq = total * total
        part = part_ref[...]
        for j in range(total.shape[1] // LANES):
            part = part + sq[:, j * LANES:(j + 1) * LANES]
        part_ref[...] = part

    def line_side(i):
        rows, cs = line_at(i, 1 - high, 3)
        return remote(acc.at[:, :, rows, cs], lside.at[i], line_send.at[1], line_recv.at[1, line_ring(i)], side_peer)

    def line_mid(i):
        rows, cs = line_at(i, 2 - 2 * high, 2)
        return remote(acc.at[:, :, rows, cs], lmid.at[i], line_send.at[2], line_recv.at[2, line_ring(i)], mid_peer)

    def line_back(i):
        rows, cs = line_at(i, 3 * high, 1)
        return remote(acc.at[:, :, rows, cs], lback.at[i], line_send.at[3], line_recv.at[3, line_ring(i)], side_peer)

    def line_one(i, h):
        rows, cs = line_at(i, z, 1)
        src = acc.at[:, 1 - x, rows, cs] if h == 0 else acc.at[1 - y, :, rows, cs]
        return remote(src, lone.at[i], line_send.at[4], line_recv.at[4, line_ring(i)], (x_peer, y_peer)[h])

    def line_two(i, h):
        rows, cs = line_at(i, z, 1)
        src = acc.at[1 - y, x, rows, cs] if h == 0 else acc.at[y, 1 - x, rows, cs]
        return remote(src, ltwo.at[i], line_send.at[5], line_recv.at[5, line_ring(i)], (y_peer, x_peer)[h])

    def gather_side(i):
        rows, cs = line_at(i, 3 * high, 1)
        return remote(mean_out.at[rows, cs], mean_out.at[rows, cs], line_send.at[6], line_recv.at[6, line_ring(i)], side_peer)

    def gather_mid(i):
        rows, cs = line_at(i, 2 * high, 2)
        return remote(mean_out.at[rows, cs], mean_out.at[rows, cs], line_send.at[7], line_recv.at[7, line_ring(i)], mid_peer)

    def gather_back(i):
        rows, cs = line_at(i, 1 - high, 3)
        return remote(mean_out.at[rows, cs], mean_out.at[rows, cs], line_send.at[8], line_recv.at[8, line_ring(i)], side_peer)

    def either_way(i, do):
        @pl.when(lax.rem(i, 2) == 0)
        def _():
            do(0)

        @pl.when(lax.rem(i, 2) == 1)
        def _():
            do(1)

    def line_stage_0(i):
        rows, cs = line_at(i)
        load_line(i).wait()
        slot = lax.rem(i, SLOTS)
        take(lown.at[slot], line_recv.at[0, line_ring(i)])
        acc[:, :, rows, cs] = acc[:, :, rows, cs] + lown[slot]

        @pl.when(is_end)
        def _():
            line_side(i).start()

    def line_stage_1(i):
        @pl.when(is_mid)
        def _():
            rows, cs = line_at(i, 1 - high, 3)
            take(lside.at[i], line_recv.at[1, line_ring(i)])
            acc[:, :, rows, cs] = acc[:, :, rows, cs] + lside[i]
            line_mid(i).start()

    def line_stage_2(i):
        @pl.when(is_mid)
        def _():
            rows, cs = line_at(i, 2 * high, 2)
            take(lmid.at[i], line_recv.at[2, line_ring(i)])
            acc[:, :, rows, cs] = acc[:, :, rows, cs] + lmid[i]
            line_back(i).start()

    def line_stage_3(i):
        @pl.when(is_end)
        def _():
            rows, cs = line_at(i, 3 * high, 1)
            take(lback.at[i], line_recv.at[3, line_ring(i)])
            acc[:, :, rows, cs] = acc[:, :, rows, cs] + lback[i]

        either_way(i, lambda h: line_one(i, h).start())

    def line_stage_4(i):
        rows, cs = line_at(i, z, 1)
        take(lone.at[i], line_recv.at[4, line_ring(i)])

        def add(h):
            if h == 0:
                acc[:, x, rows, cs] = acc[:, x, rows, cs] + lone[i]
            else:
                acc[y, :, rows, cs] = acc[y, :, rows, cs] + lone[i]
            line_two(i, h).start()

        either_way(i, add)

    def line_stage_5(i):
        rows, cs = line_at(i, z, 1)
        take(ltwo.at[i], line_recv.at[5, line_ring(i)])
        mean_out[rows, cs] = (acc[y, x, rows, cs] + ltwo[i]) * inv_count

        @pl.when(is_end)
        def _():
            gather_side(i).start()

    def line_stage_6(i):
        @pl.when(is_mid)
        def _():
            take(ltwo.at[i], line_recv.at[6, line_ring(i)])
            gather_mid(i).start()

    def line_stage_7(i):
        @pl.when(is_mid)
        def _():
            take(lone.at[i], line_recv.at[7, line_ring(i)])
            gather_back(i).start()
            rows, cs = line_at(i)
            add_squares(sq_line, mean_out[rows, cs])

    def line_stage_8(i):
        @pl.when(is_end)
        def _():
            take(lside.at[i, 0, 0], line_recv.at[8, line_ring(i)])

    line_stages = (line_stage_0, line_stage_1, line_stage_2, line_stage_3, line_stage_4, line_stage_5, line_stage_6,
                   line_stage_7, line_stage_8)

    norm_core = remote(nsend, nacc, nsend_sem.at[0], nrecv_sem.at[0], core_peer)
    norm_one = remote(nacc.at[:, 1 - x], none, nsend_sem.at[1], nrecv_sem.at[1], x_peer)
    norm_two = remote(nacc.at[1 - y, x], ntwo, nsend_sem.at[2], nrecv_sem.at[2], y_peer)
    norm_side = remote(nacc.at[y, x], nzin, nsend_sem.at[3], nrecv_sem.at[3], side_peer)
    norm_mid = remote(nacc.at[y, x], nzmid, nsend_sem.at[4], nrecv_sem.at[4], mid_peer)
    norm_back = remote(nzin, nzin, nsend_sem.at[5], nrecv_sem.at[3], side_peer)
    def state_parts(j):
        split = emb_state[j].shape[0]
        return ((emb_state[j], state_out[j].at[pl.ds(0, split)]),
                (mat_state[j], state_out[j].at[pl.ds(split, mat_state[j].shape[0])]))

    def body(t, carry):
        @pl.when(t + CORE_AHEAD < rounds)
        def _():
            send_core(t + CORE_AHEAD)

        @pl.when(t + AHEAD < rounds)
        def _():
            load_own(t + AHEAD)

        early = t + CORE_AHEAD

        @pl.when((lax.rem(early, LINE_RATE) == 0) & (early < lines * LINE_RATE))
        def _():
            line_core(lax.div(early, LINE_RATE)).start()
            load_line(lax.div(early, LINE_RATE)).start()

        @pl.when(t < rounds)
        def _():
            rb, _, wide, _ = piece(t)
            slot = lax.rem(t, SLOTS)
            take(own.at[slot], own_sem.at[slot])
            take(own.at[slot], core_recv.at[lax.rem(t, CORE_RING)])
            for h in range(2):
                acc[:, :, rb, wide[h]] = acc[:, :, rb, wide[h]] + own[slot, h]
                one_copy(t, h).start()

        q1 = t - LAG_ONE

        @pl.when((q1 >= 0) & (q1 < rounds))
        def _():
            rb, inner, wide, cs = piece(q1)
            one_copy(q1, 0).wait_recv()
            acc[:, x, rb, wide[0]] = acc[:, x, rb, wide[0]] + one[0, :, inner, cs]
            two_copy(q1, 0).start()
            one_copy(q1, 1).wait_recv()
            acc[y, :, rb, wide[1]] = acc[y, :, rb, wide[1]] + one[1, :, inner, cs]
            two_copy(q1, 1).start()

        q2 = t - LAG_TWO

        @pl.when((q2 >= 0) & (q2 < rounds))
        def _():
            rb, inner, wide, cs = piece(q2)
            for h in range(2):
                two_copy(q2, h).wait_recv()
                acc[y, x, rb, wide[h]] = acc[y, x, rb, wide[h]] + two[h, inner, cs]

                @pl.when(is_end)
                def _(h=h):
                    side_copy(q2, h).start()

        q3 = t - LAG_SIDE

        @pl.when(is_mid & (q3 >= 0) & (q3 < rounds))
        def _():
            rb, _, wide, _ = piece(q3)
            for h in range(2):
                side_copy(q3, h).wait_recv()
                acc[y, x, rb, wide[h]] = acc[y, x, rb, wide[h]] + mean_out[rb, wide[h]]
                mid_copy(q3, h).start()

        q4 = t - LAG_MID

        @pl.when(is_mid & (q4 >= 0) & (q4 < rounds))
        def _():
            rb, inner, wide, _ = piece(q4)
            for h in range(2):
                mid_copy(q4, h).wait_recv()
                total = (acc[y, x, rb, wide[h]] + zmid[inner, wide[h]]) * inv_count
                mean_out[rb, wide[h]] = total
                back_copy(q4, h).start()
                add_squares(sq_main, total)

        q5 = t - LAG_BACK

        @pl.when(is_end & (q5 >= 0) & (q5 < rounds))
        def _():
            for h in range(2):
                back_copy(q5, h).wait_recv()

        for k, stage in enumerate(line_stages):
            late = t - k * LINE_STEP

            @pl.when((late >= 0) & (late < lines * LINE_RATE) & (lax.rem(late, LINE_RATE) == 0))
            def _(late=late, stage=stage):
                stage(lax.div(late, LINE_RATE))

        @pl.when(t == STATE_ROUND)
        def _():
            for j in range(3):
                for src, dst in state_parts(j):
                    pltpu.make_async_copy(src, dst, state_sem.at[j]).start()

        @pl.when(t == NORM_START - NORM_STEP)
        def _():
            norm_load.wait()
            shard = nacc.shape[4]
            for yy in range(2):
                for xx in range(2):
                    at = (4 * yy + 2 * xx) * shard
                    first = norm_all[:, :, at:at + shard]
                    second = norm_all[:, :, at + shard:at + 2 * shard]
                    nsend[yy, xx] = jnp.where(c == 0, second, first)
                    nown[yy, xx] = jnp.where(c == 0, first, second)
            norm_core.start()

        @pl.when(t == NORM_START)
        def _():
            norm_core.wait_recv()
            nacc[...] = nacc[...] + nown[...]
            norm_one.start()

        @pl.when(t == NORM_START + NORM_STEP)
        def _():
            norm_one.wait_recv()
            nacc[:, x] = nacc[:, x] + none[...]
            norm_two.start()

        @pl.when(t == NORM_START + 2 * NORM_STEP)
        def _():
            norm_two.wait_recv()
            nacc[y, x] = nacc[y, x] + ntwo[...]

            @pl.when(is_end)
            def _():
                norm_side.start()

        @pl.when(is_mid & (t == NORM_START + 3 * NORM_STEP))
        def _():
            norm_side.wait_recv()
            nacc[y, x] = nacc[y, x] + nzin[...]
            norm_mid.start()

        @pl.when(is_mid & (t == NORM_START + 4 * NORM_STEP))
        def _():
            norm_mid.wait_recv()
            nzin[...] = (nacc[y, x] + nzmid[...]) * inv_count
            norm_back.start()

        @pl.when(is_end & (t == NORM_START + 5 * NORM_STEP))
        def _():
            norm_back.wait_recv()

        @pl.when(t == NORM_START + 6 * NORM_STEP)
        def _():
            for j in range(norm_out.shape[0]):
                norm_out[j:j + 1, :] = nzin[j]
            norm_total = nzin[...]
            norm_sq = jnp.sum(norm_total * norm_total)
            corner = [lax.broadcasted_iota(jnp.int32, sq_line.shape, d) == 0 for d in range(2)]
            sq_norm = jnp.where(corner[0] & corner[1], norm_sq, 0.0)
            sq_all[0] = sq_norm

        return carry

    lax.fori_loop(0, rounds + LAG_BACK, body, 0)

    for j in range(3):
        take(state_out[j], state_sem.at[j])
    scale_copy = remote(scale_out, scale_out, scale_send, scale_recv, side_peer)

    @pl.when(is_mid)
    def _():
        sq_main[...] = sq_main[...] + sq_line[...] + sq_all[0]
        for step in range(1, 8):
            remote(sq_main, sq_all.at[1 + f], sq_send, sq_recv, (z, lax.rem(f + step, 8))).start()
        sq_all[1 + f] = sq_main[...]
        seven = sq_all.at[pl.ds(0, 7)]
        take(seven, sq_recv)
        square = sq_all[1]
        for j in range(2, 9):
            square = square + sq_all[j]
        scale_out[...] = jnp.minimum(1.0, CLIP_NORM / jnp.sqrt(jnp.broadcast_to(jnp.sum(square), square.shape)))
        scale_copy.start()
        take(seven, sq_send)

    @pl.when(is_end)
    def _():
        scale_copy.wait_recv()

    take(acc.at[:, :, pl.ds(0, one.shape[2])], core_send)
    for h in range(2):
        take(one.at[h], one_send.at[h])
        take(two.at[h], two_send.at[h])
    take(acc.at[:, :, pl.ds(0, 8 * LINE_BLOCKS)], line_send.at[0])
    take(lone, line_send.at[4])
    take(ltwo, line_send.at[5])
    norm_core.wait_send()
    norm_one.wait_send()
    norm_two.wait_send()

    @pl.when(is_end)
    def _():
        take(zmid, side_send)
        take(lside, line_send.at[1])
        take(ltwo, line_send.at[6])
        norm_side.wait_send()

    @pl.when(is_mid)
    def _():
        take(zmid, mid_send)
        take(zmid, back_send)
        take(lmid, line_send.at[2])
        take(lback, line_send.at[3])
        take(lone, line_send.at[7])
        take(lside.at[:, 0, 0], line_send.at[8])
        norm_mid.wait_send()
        norm_back.wait_send()
        scale_copy.wait_send()


def adam_kernel(scale_ref, mean_ref, norm_ref, *refs):
    ins, outs, news, sems = refs[:6], refs[6:18], refs[18:30], refs[30]
    clip = scale_ref[0:1, 0:1]
    rate = LEARN_RATE / (1.0 - BETA_ONE ** ADAM_STEP)
    bias_two = 1.0 / (1.0 - BETA_TWO ** ADAM_STEP)
    emb_rows = outs[0].shape[0]

    def update(group, grad_ref, states, source, start, rows, decay_rate):
        width = grad_ref.shape[1]
        cols = ADAM_COLS if width % ADAM_COLS == 0 else width
        at, here = pl.ds(start, rows), pl.ds(source + start, rows)
        for left in range(0, width, cols):
            cs = pl.ds(left, cols)
            grad = grad_ref[here, cs] * clip
            param, mom, var = (ref[here, cs] for ref in states)
            new_mom = BETA_ONE * mom + (1.0 - BETA_ONE) * grad
            new_var = BETA_TWO * var + (1.0 - BETA_TWO) * grad * grad
            move = rate * new_mom / (jnp.sqrt(new_var * bias_two) + ADAM_EPS)
            new_param = (1.0 - LEARN_RATE * decay_rate) * param - move
            for ref, value in zip(news[4 * group:4 * group + 4], (new_param, new_mom, new_var, new_param)):
                ref[at, cs] = value.astype(ref.dtype)
        for k in range(4 * group, 4 * group + 4):
            pltpu.make_async_copy(news[k].at[at], outs[k].at[at], sems.at[k]).start()

    update(2, norm_ref, ins[3:], 0, 0, norm_ref.shape[0], 0.0)
    update(1, mean_ref, ins[:3], emb_rows, 0, outs[4].shape[0], WEIGHT_DECAY)

    def some_rows(r, carry):
        update(0, mean_ref, ins[:3], 0, pl.multiple_of(r * ADAM_ROWS, ADAM_ROWS), ADAM_ROWS, WEIGHT_DECAY)
        return carry

    lax.fori_loop(0, emb_rows // ADAM_ROWS, some_rows, 0)
    for k in range(12):
        pltpu.make_async_copy(outs[k], outs[k], sems.at[k]).wait()


def solution(mesh):
    dev_count = mesh.shape["dp"] * mesh.shape["fsdp"]

    def local_step(emb_grad, mat_grad, norm_grad, emb_param, emb_mom, emb_var, mat_param, mat_mom, mat_var, norm_param, norm_mom, norm_var):
        width = emb_grad.shape[3]
        emb_rows, mat_rows = emb_param.shape[0], mat_param.shape[0]
        count, shard = norm_param.shape
        emb_in = emb_grad.reshape(2, 2, 2, emb_rows, width)
        mat_in = mat_grad.reshape(2, 2, 2, mat_rows, width)
        norm_in = norm_grad.reshape(count, 1, norm_grad.shape[3])
        rows = emb_rows + mat_rows
        main_rows = rows - 8 * LINE_BLOCKS
        rounds = main_rows // 8 * SPLIT
        half = width // 2
        lines = LINE_BLOCKS * LINE_SPLIT
        quarter = width // LINE_SPLIT // 4
        any_spec = pl.BlockSpec(memory_space=pl.ANY)
        vmem_spec = pl.BlockSpec(memory_space=pltpu.VMEM)
        dma = pltpu.SemaphoreType.DMA
        vmem = lambda *shape: pltpu.VMEM(shape, F32)
        mean, norm_mean, scale, param, mom, var = pl.pallas_call(
            functools.partial(reduce_kernel, 1.0 / dev_count),
            out_shape=(
                vmem(rows, width),
                vmem(count, shard),
                vmem(8, LANES),
            ) + (vmem(rows, width),) * 3,
            in_specs=[any_spec] * 9,
            out_specs=(vmem_spec,) * 6,
            scratch_shapes=[
                vmem(2, 2, rows, width),
                vmem(SLOTS, 2, 2, 2, 8, half // SPLIT),
                vmem(2, 2, main_rows, half),
                vmem(2, main_rows, half),
                vmem(main_rows, width),
                vmem(SLOTS, 2, 2, 8, 4 * quarter),
                vmem(lines, 2, 2, 8, 3 * quarter),
                vmem(lines, 2, 2, 8, 2 * quarter),
                vmem(lines, 2, 2, 8, quarter),
                vmem(lines, 2, 8, quarter),
                vmem(lines, 8, quarter),
                vmem(*norm_in.shape),
                vmem(2, 2, count, 1, shard),
                vmem(2, 2, count, 1, shard),
                vmem(2, 2, count, 1, shard),
                vmem(2, count, 1, shard),
                vmem(count, 1, shard),
                vmem(count, 1, shard),
                vmem(count, 1, shard),
                vmem(8, LANES),
                vmem(8, LANES),
                vmem(9, 8, LANES),
                dma, dma((CORE_RING,)), dma((SLOTS,)),
                dma((2,)), dma((2, RING)), dma((2,)), dma((2, RING)),
                dma, dma((2, RING)), dma, dma((2, RING)), dma,
                dma((SLOTS,)), dma((9,)), dma((9, LINE_RING)),
                dma, dma((6,)), dma((6,)), dma, dma, dma, dma, dma((3,)),
            ],
            compiler_params=pltpu.CompilerParams(collective_id=0, has_side_effects=True, vmem_limit_bytes=VMEM_KIB << 10),
            name="reduce_gradients",
        )(*(pltpu.with_memory_space_constraint(a, pltpu.HBM) for a in (
            emb_in, mat_in, norm_in, emb_param, emb_mom, emb_var, mat_param, mat_mom, mat_var)))
        shapes = []
        for like in (emb_param, mat_param, norm_param):
            shapes += [jax.ShapeDtypeStruct(like.shape, F32)] * 3 + [jax.ShapeDtypeStruct(like.shape, jnp.bfloat16)]
        return pl.pallas_call(
            adam_kernel,
            out_shape=tuple(shapes),
            in_specs=[vmem_spec] * 9,
            out_specs=(any_spec,) * 12,
            scratch_shapes=[pltpu.VMEM(like.shape, like.dtype) for like in shapes] + [dma((12,))],
            compiler_params=pltpu.CompilerParams(vmem_limit_bytes=ADAM_MIB << 20),
            name="adam",
        )(scale, mean, norm_mean, param, mom, var, norm_param, norm_mom, norm_var)

    grad_spec = P("dp", "fsdp", None, None)
    row_spec = P("fsdp", None)
    col_spec = P(None, "fsdp")
    in_list = (grad_spec, grad_spec, grad_spec, row_spec, row_spec, row_spec, row_spec, row_spec, row_spec, col_spec, col_spec, col_spec)
    out_list = (row_spec, row_spec, row_spec, row_spec, row_spec, row_spec, row_spec, row_spec, col_spec, col_spec, col_spec, col_spec)
    return jax.shard_map(local_step, mesh=mesh, in_specs=in_list, out_specs=out_list, check_vma=False)
```

```python
import functools

import jax
import jax.numpy as jnp
from jax import lax
from jax.experimental import pallas as pl
from jax.experimental.pallas import tpu as pltpu
from jax.sharding import PartitionSpec as P

LEARN_RATE = 0.003
BETA_ONE = 0.9
BETA_TWO = 0.95
ADAM_EPS = 1e-8
WEIGHT_DECAY = 0.1
CLIP_NORM = 1.0
ADAM_STEP = 10

MESH = pl.DeviceIdType.MESH
F32 = jnp.float32
LANES = 128
SPLIT = 3
AHEAD = 2
SLOTS = 4
CORE_RING, RING, LINE_RING = 12, 12, 5
STATE_ROUND = 16
CORE_AHEAD = 4
LAG_ONE, LAG_TWO, LAG_SIDE, LAG_MID, LAG_BACK = 3, 6, 9, 12, 15
NORM_START, NORM_STEP = 12, 6
LINE_BLOCKS = 5
LINE_SPLIT = 3
LINE_RATE, LINE_STEP = 5, 3
ADAM_ROWS, ADAM_COLS = 16, 512
VMEM_KIB, ADAM_MIB = 45568, 20


def reduce_kernel(inv_count, emb_ref, mat_ref, norm_ref, *refs):
    emb_state, mat_state, state_out = refs[0:3], refs[3:6], refs[9:12]
    mean_out, norm_out, scale_out = refs[6:9]
    (acc, own, one, two, zmid, lown, lside, lmid, lback, lone, ltwo,
     norm_all, nsend, nown, nacc, none, ntwo, nzin, nzmid, sq_main, sq_line, sq_all,
     core_send, core_recv, own_sem, one_send, one_recv, two_send, two_recv,
     side_send, side_recv, mid_send, mid_recv, back_send,
     lown_sem, line_send, line_recv, norm_sem, nsend_sem, nrecv_sem, sq_send, sq_recv, scale_send, scale_recv, state_sem) = refs[12:]
    z = lax.axis_index("dp")
    f = lax.axis_index("fsdp")
    y, x, c = f // 4, (f // 2) % 2, f % 2
    width = acc.shape[3]
    half = width // 2
    cols = half // SPLIT
    emb_blocks = emb_ref.shape[3] // 8
    rounds = one.shape[2] // 8 * SPLIT
    emb_rounds = (emb_blocks - LINE_BLOCKS) * SPLIT
    lines = lside.shape[0]
    lwidth = width // LINE_SPLIT
    quarter = lwidth // 4
    is_end = (z == 0) | (z == 3)
    is_mid = (z == 1) | (z == 2)
    high = z // 2
    side = z + 1 - 2 * (z % 2)
    core_peer = (z, y * 4 + x * 2 + 1 - c)
    x_peer = (z, y * 4 + (1 - x) * 2 + c)
    y_peer = (z, (1 - y) * 4 + x * 2 + c)
    side_peer = (side, f)
    mid_peer = (lax.rem(3 - z, 4), f)

    def remote(src, dst, send_sem, recv_sem, peer):
        return pltpu.make_async_remote_copy(src, dst, send_sem, recv_sem, device_id=peer, device_id_type=MESH)

    def take(ref, sem):
        pltpu.make_async_copy(ref, ref, sem).wait()

    def ring(q):
        return lax.rem(q, RING)

    def line_ring(i):
        return lax.rem(i, LINE_RING)

    def piece(q):
        block, sub = lax.div(q, SPLIT), lax.rem(q, SPLIT) * cols
        rows = pl.ds(pl.multiple_of((block + LINE_BLOCKS) * 8, 8), 8)
        inner = pl.ds(pl.multiple_of(block * 8, 8), 8)
        wide = [pl.ds(pl.multiple_of(sub + h * half, LANES), cols) for h in range(2)]
        return rows, inner, wide, pl.ds(pl.multiple_of(sub, LANES), cols)

    def mat_rows(q):
        return pl.ds(pl.multiple_of((lax.div(q, SPLIT) + LINE_BLOCKS - emb_blocks) * 8, 8), 8)

    def from_emb_or_mat(q, do):
        rows, _, wide, _ = piece(q)

        @pl.when(q < emb_rounds)
        def _():
            for h in range(2):
                do(emb_ref, rows, h, wide[h])

        @pl.when(q >= emb_rounds)
        def _():
            for h in range(2):
                do(mat_ref, mat_rows(q), h, wide[h])

    def load_own(q):
        slot = lax.rem(q, SLOTS)
        from_emb_or_mat(q, lambda ref, rows, h, cs: pltpu.make_async_copy(
            ref.at[:, :, c, rows, cs], own.at[slot, h], own_sem.at[slot]).start())

    def send_core(q):
        rb = piece(q)[0]
        from_emb_or_mat(q, lambda ref, rows, h, cs: remote(
            ref.at[:, :, 1 - c, rows, cs], acc.at[:, :, rb, cs], core_send, core_recv.at[lax.rem(q, CORE_RING)], core_peer).start())

    def line_at(i, start=0, size=4):
        rows = pl.ds(pl.multiple_of(lax.div(i, LINE_SPLIT) * 8, 8), 8)
        return rows, pl.ds(pl.multiple_of(lax.rem(i, LINE_SPLIT) * lwidth + start * quarter, LANES), size * quarter)

    def load_line(i):
        rows, cs = line_at(i)
        slot = lax.rem(i, SLOTS)
        return pltpu.make_async_copy(emb_ref.at[:, :, c, rows, cs], lown.at[slot], lown_sem.at[slot])

    def line_core(i):
        rows, cs = line_at(i)
        return remote(emb_ref.at[:, :, 1 - c, rows, cs], acc.at[:, :, rows, cs], line_send.at[0], line_recv.at[0, line_ring(i)], core_peer)

    norm_load = pltpu.make_async_copy(norm_ref, norm_all, norm_sem)
    norm_load.start()
    for q in range(AHEAD):
        load_own(jnp.int32(q))
    load_line(jnp.int32(0)).start()

    barrier = pltpu.get_barrier_semaphore()
    pl.semaphore_signal(barrier, inc=1, device_id=side_peer, device_id_type=MESH)

    @pl.when(is_mid)
    def _():
        for step in range(1, 8):
            pl.semaphore_signal(barrier, inc=1, device_id=(z, lax.rem(f + step, 8)), device_id_type=MESH)
        pl.semaphore_signal(barrier, inc=1, device_id=mid_peer, device_id_type=MESH)
        pl.semaphore_wait(barrier, 9)

    @pl.when(is_end)
    def _():
        for peer in (core_peer, x_peer, y_peer):
            pl.semaphore_signal(barrier, inc=1, device_id=peer, device_id_type=MESH)
        pl.semaphore_wait(barrier, 4)

    for q in range(CORE_AHEAD):
        send_core(jnp.int32(q))
        if q == 0:
            line_core(jnp.int32(0)).start()

    sq_main[...] = jnp.zeros_like(sq_main)
    sq_line[...] = jnp.zeros_like(sq_line)

    def one_copy(q, h):
        rb, inner, wide, cs = piece(q)
        src = acc.at[:, 1 - x, rb, wide[0]] if h == 0 else acc.at[1 - y, :, rb, wide[1]]
        return remote(src, one.at[h, :, inner, cs], one_send.at[h], one_recv.at[h, ring(q)], (x_peer, y_peer)[h])

    def two_copy(q, h):
        rb, inner, wide, cs = piece(q)
        src = acc.at[1 - y, x, rb, wide[0]] if h == 0 else acc.at[y, 1 - x, rb, wide[1]]
        return remote(src, two.at[h, inner, cs], two_send.at[h], two_recv.at[h, ring(q)], (y_peer, x_peer)[h])

    def side_copy(q, h):
        rb, _, wide, _ = piece(q)
        return remote(acc.at[y, x, rb, wide[h]], mean_out.at[rb, wide[h]], side_send, side_recv.at[h, ring(q)], side_peer)

    def mid_copy(q, h):
        rb, inner, wide, _ = piece(q)
        return remote(acc.at[y, x, rb, wide[h]], zmid.at[inner, wide[h]], mid_send, mid_recv.at[h, ring(q)], mid_peer)

    def back_copy(q, h):
        rb, _, wide, _ = piece(q)
        return remote(mean_out.at[rb, wide[h]], mean_out.at[rb, wide[h]], back_send, side_recv.at[h, ring(q)], side_peer)

    def add_squares(part_ref, total):
        sq = total * total
        part = part_ref[...]
        for j in range(total.shape[1] // LANES):
            part = part + sq[:, j * LANES:(j + 1) * LANES]
        part_ref[...] = part

    def line_side(i):
        rows, cs = line_at(i, 1 - high, 3)
        return remote(acc.at[:, :, rows, cs], lside.at[i], line_send.at[1], line_recv.at[1, line_ring(i)], side_peer)

    def line_mid(i):
        rows, cs = line_at(i, 2 - 2 * high, 2)
        return remote(acc.at[:, :, rows, cs], lmid.at[i], line_send.at[2], line_recv.at[2, line_ring(i)], mid_peer)

    def line_back(i):
        rows, cs = line_at(i, 3 * high, 1)
        return remote(acc.at[:, :, rows, cs], lback.at[i], line_send.at[3], line_recv.at[3, line_ring(i)], side_peer)

    def line_one(i, h):
        rows, cs = line_at(i, z, 1)
        src = acc.at[:, 1 - x, rows, cs] if h == 0 else acc.at[1 - y, :, rows, cs]
        return remote(src, lone.at[i], line_send.at[4], line_recv.at[4, line_ring(i)], (x_peer, y_peer)[h])

    def line_two(i, h):
        rows, cs = line_at(i, z, 1)
        src = acc.at[1 - y, x, rows, cs] if h == 0 else acc.at[y, 1 - x, rows, cs]
        return remote(src, ltwo.at[i], line_send.at[5], line_recv.at[5, line_ring(i)], (y_peer, x_peer)[h])

    def gather_side(i):
        rows, cs = line_at(i, 3 * high, 1)
        return remote(mean_out.at[rows, cs], mean_out.at[rows, cs], line_send.at[6], line_recv.at[6, line_ring(i)], side_peer)

    def gather_mid(i):
        rows, cs = line_at(i, 2 * high, 2)
        return remote(mean_out.at[rows, cs], mean_out.at[rows, cs], line_send.at[7], line_recv.at[7, line_ring(i)], mid_peer)

    def gather_back(i):
        rows, cs = line_at(i, 1 - high, 3)
        return remote(mean_out.at[rows, cs], mean_out.at[rows, cs], line_send.at[8], line_recv.at[8, line_ring(i)], side_peer)

    def either_way(i, do):
        @pl.when(lax.rem(i, 2) == 0)
        def _():
            do(0)

        @pl.when(lax.rem(i, 2) == 1)
        def _():
            do(1)

    def line_stage_0(i):
        rows, cs = line_at(i)
        load_line(i).wait()
        slot = lax.rem(i, SLOTS)
        take(lown.at[slot], line_recv.at[0, line_ring(i)])
        acc[:, :, rows, cs] = acc[:, :, rows, cs] + lown[slot]

        @pl.when(is_end)
        def _():
            line_side(i).start()

    def line_stage_1(i):
        @pl.when(is_mid)
        def _():
            rows, cs = line_at(i, 1 - high, 3)
            take(lside.at[i], line_recv.at[1, line_ring(i)])
            acc[:, :, rows, cs] = acc[:, :, rows, cs] + lside[i]
            line_mid(i).start()

    def line_stage_2(i):
        @pl.when(is_mid)
        def _():
            rows, cs = line_at(i, 2 * high, 2)
            take(lmid.at[i], line_recv.at[2, line_ring(i)])
            acc[:, :, rows, cs] = acc[:, :, rows, cs] + lmid[i]
            line_back(i).start()

    def line_stage_3(i):
        @pl.when(is_end)
        def _():
            rows, cs = line_at(i, 3 * high, 1)
            take(lback.at[i], line_recv.at[3, line_ring(i)])
            acc[:, :, rows, cs] = acc[:, :, rows, cs] + lback[i]

        either_way(i, lambda h: line_one(i, h).start())

    def line_stage_4(i):
        rows, cs = line_at(i, z, 1)
        take(lone.at[i], line_recv.at[4, line_ring(i)])

        def add(h):
            if h == 0:
                acc[:, x, rows, cs] = acc[:, x, rows, cs] + lone[i]
            else:
                acc[y, :, rows, cs] = acc[y, :, rows, cs] + lone[i]
            line_two(i, h).start()

        either_way(i, add)

    def line_stage_5(i):
        rows, cs = line_at(i, z, 1)
        take(ltwo.at[i], line_recv.at[5, line_ring(i)])
        mean_out[rows, cs] = (acc[y, x, rows, cs] + ltwo[i]) * inv_count

        @pl.when(is_end)
        def _():
            gather_side(i).start()

    def line_stage_6(i):
        @pl.when(is_mid)
        def _():
            take(ltwo.at[i], line_recv.at[6, line_ring(i)])
            gather_mid(i).start()

    def line_stage_7(i):
        @pl.when(is_mid)
        def _():
            take(lone.at[i], line_recv.at[7, line_ring(i)])
            gather_back(i).start()
            rows, cs = line_at(i)
            add_squares(sq_line, mean_out[rows, cs])

    def line_stage_8(i):
        @pl.when(is_end)
        def _():
            take(lside.at[i, 0, 0], line_recv.at[8, line_ring(i)])

    line_stages = (line_stage_0, line_stage_1, line_stage_2, line_stage_3, line_stage_4, line_stage_5, line_stage_6,
                   line_stage_7, line_stage_8)

    norm_core = remote(nsend, nacc, nsend_sem.at[0], nrecv_sem.at[0], core_peer)
    norm_one = remote(nacc.at[:, 1 - x], none, nsend_sem.at[1], nrecv_sem.at[1], x_peer)
    norm_two = remote(nacc.at[1 - y, x], ntwo, nsend_sem.at[2], nrecv_sem.at[2], y_peer)
    norm_side = remote(nacc.at[y, x], nzin, nsend_sem.at[3], nrecv_sem.at[3], side_peer)
    norm_mid = remote(nacc.at[y, x], nzmid, nsend_sem.at[4], nrecv_sem.at[4], mid_peer)
    norm_back = remote(nzin, nzin, nsend_sem.at[5], nrecv_sem.at[3], side_peer)
    def state_parts(j):
        split = emb_state[j].shape[0]
        return ((emb_state[j], state_out[j].at[pl.ds(0, split)]),
                (mat_state[j], state_out[j].at[pl.ds(split, mat_state[j].shape[0])]))

    def body(t, carry):
        @pl.when(t + CORE_AHEAD < rounds)
        def _():
            send_core(t + CORE_AHEAD)

        @pl.when(t + AHEAD < rounds)
        def _():
            load_own(t + AHEAD)

        early = t + CORE_AHEAD

        @pl.when((lax.rem(early, LINE_RATE) == 0) & (early < lines * LINE_RATE))
        def _():
            line_core(lax.div(early, LINE_RATE)).start()
            load_line(lax.div(early, LINE_RATE)).start()

        @pl.when(t < rounds)
        def _():
            rb, _, wide, _ = piece(t)
            slot = lax.rem(t, SLOTS)
            take(own.at[slot], own_sem.at[slot])
            take(own.at[slot], core_recv.at[lax.rem(t, CORE_RING)])
            for h in range(2):
                acc[:, :, rb, wide[h]] = acc[:, :, rb, wide[h]] + own[slot, h]
                one_copy(t, h).start()

        q1 = t - LAG_ONE

        @pl.when((q1 >= 0) & (q1 < rounds))
        def _():
            rb, inner, wide, cs = piece(q1)
            one_copy(q1, 0).wait_recv()
            acc[:, x, rb, wide[0]] = acc[:, x, rb, wide[0]] + one[0, :, inner, cs]
            two_copy(q1, 0).start()
            one_copy(q1, 1).wait_recv()
            acc[y, :, rb, wide[1]] = acc[y, :, rb, wide[1]] + one[1, :, inner, cs]
            two_copy(q1, 1).start()

        q2 = t - LAG_TWO

        @pl.when((q2 >= 0) & (q2 < rounds))
        def _():
            rb, inner, wide, cs = piece(q2)
            for h in range(2):
                two_copy(q2, h).wait_recv()
                acc[y, x, rb, wide[h]] = acc[y, x, rb, wide[h]] + two[h, inner, cs]

                @pl.when(is_end)
                def _(h=h):
                    side_copy(q2, h).start()

        q3 = t - LAG_SIDE

        @pl.when(is_mid & (q3 >= 0) & (q3 < rounds))
        def _():
            rb, _, wide, _ = piece(q3)
            for h in range(2):
                side_copy(q3, h).wait_recv()
                acc[y, x, rb, wide[h]] = acc[y, x, rb, wide[h]] + mean_out[rb, wide[h]]
                mid_copy(q3, h).start()

        q4 = t - LAG_MID

        @pl.when(is_mid & (q4 >= 0) & (q4 < rounds))
        def _():
            rb, inner, wide, _ = piece(q4)
            for h in range(2):
                mid_copy(q4, h).wait_recv()
                total = (acc[y, x, rb, wide[h]] + zmid[inner, wide[h]]) * inv_count
                mean_out[rb, wide[h]] = total
                back_copy(q4, h).start()
                add_squares(sq_main, total)

        q5 = t - LAG_BACK

        @pl.when(is_end & (q5 >= 0) & (q5 < rounds))
        def _():
            for h in range(2):
                back_copy(q5, h).wait_recv()

        for k, stage in enumerate(line_stages):
            late = t - k * LINE_STEP

            @pl.when((late >= 0) & (late < lines * LINE_RATE) & (lax.rem(late, LINE_RATE) == 0))
            def _(late=late, stage=stage):
                stage(lax.div(late, LINE_RATE))

        @pl.when(t == STATE_ROUND)
        def _():
            for j in range(3):
                for src, dst in state_parts(j):
                    pltpu.make_async_copy(src, dst, state_sem.at[j]).start()

        @pl.when(t == NORM_START - NORM_STEP)
        def _():
            norm_load.wait()
            shard = nacc.shape[4]
            for yy in range(2):
                for xx in range(2):
                    at = (4 * yy + 2 * xx) * shard
                    first = norm_all[:, :, at:at + shard]
                    second = norm_all[:, :, at + shard:at + 2 * shard]
                    nsend[yy, xx] = jnp.where(c == 0, second, first)
                    nown[yy, xx] = jnp.where(c == 0, first, second)
            norm_core.start()

        @pl.when(t == NORM_START)
        def _():
            norm_core.wait_recv()
            nacc[...] = nacc[...] + nown[...]
            norm_one.start()

        @pl.when(t == NORM_START + NORM_STEP)
        def _():
            norm_one.wait_recv()
            nacc[:, x] = nacc[:, x] + none[...]
            norm_two.start()

        @pl.when(t == NORM_START + 2 * NORM_STEP)
        def _():
            norm_two.wait_recv()
            nacc[y, x] = nacc[y, x] + ntwo[...]

            @pl.when(is_end)
            def _():
                norm_side.start()

        @pl.when(is_mid & (t == NORM_START + 3 * NORM_STEP))
        def _():
            norm_side.wait_recv()
            nacc[y, x] = nacc[y, x] + nzin[...]
            norm_mid.start()

        @pl.when(is_mid & (t == NORM_START + 4 * NORM_STEP))
        def _():
            norm_mid.wait_recv()
            nzin[...] = (nacc[y, x] + nzmid[...]) * inv_count
            norm_back.start()

        @pl.when(is_end & (t == NORM_START + 5 * NORM_STEP))
        def _():
            norm_back.wait_recv()

        @pl.when(t == NORM_START + 6 * NORM_STEP)
        def _():
            for j in range(norm_out.shape[0]):
                norm_out[j:j + 1, :] = nzin[j]
            norm_total = nzin[...]
            norm_sq = jnp.sum(norm_total * norm_total)
            corner = [lax.broadcasted_iota(jnp.int32, sq_line.shape, d) == 0 for d in range(2)]
            sq_norm = jnp.where(corner[0] & corner[1], norm_sq, 0.0)
            sq_all[0] = sq_norm

        return carry

    lax.fori_loop(0, rounds + LAG_BACK, body, 0)

    for j in range(3):
        take(state_out[j], state_sem.at[j])
    scale_copy = remote(scale_out, scale_out, scale_send, scale_recv, side_peer)

    @pl.when(is_mid)
    def _():
        sq_main[...] = sq_main[...] + sq_line[...] + sq_all[0]
        for step in range(1, 8):
            remote(sq_main, sq_all.at[1 + f], sq_send, sq_recv, (z, lax.rem(f + step, 8))).start()
        sq_all[1 + f] = sq_main[...]
        seven = sq_all.at[pl.ds(0, 7)]
        take(seven, sq_recv)
        square = sq_all[1]
        for j in range(2, 9):
            square = square + sq_all[j]
        scale_out[...] = jnp.minimum(1.0, CLIP_NORM / jnp.sqrt(jnp.broadcast_to(jnp.sum(square), square.shape)))
        scale_copy.start()
        take(seven, sq_send)

    @pl.when(is_end)
    def _():
        scale_copy.wait_recv()

    take(acc.at[:, :, pl.ds(0, one.shape[2])], core_send)
    for h in range(2):
        take(one.at[h], one_send.at[h])
        take(two.at[h], two_send.at[h])
    take(acc.at[:, :, pl.ds(0, 8 * LINE_BLOCKS)], line_send.at[0])
    take(lone, line_send.at[4])
    take(ltwo, line_send.at[5])
    norm_core.wait_send()
    norm_one.wait_send()
    norm_two.wait_send()

    @pl.when(is_end)
    def _():
        take(zmid, side_send)
        take(lside, line_send.at[1])
        take(ltwo, line_send.at[6])
        norm_side.wait_send()

    @pl.when(is_mid)
    def _():
        take(zmid, mid_send)
        take(zmid, back_send)
        take(lmid, line_send.at[2])
        take(lback, line_send.at[3])
        take(lone, line_send.at[7])
        take(lside.at[:, 0, 0], line_send.at[8])
        norm_mid.wait_send()
        norm_back.wait_send()
        scale_copy.wait_send()


def adam_kernel(scale_ref, mean_ref, norm_ref, *refs):
    ins, outs, news, sems = refs[:6], refs[6:18], refs[18:30], refs[30]
    clip = scale_ref[0:1, 0:1]
    rate = LEARN_RATE / (1.0 - BETA_ONE ** ADAM_STEP)
    bias_two = 1.0 / (1.0 - BETA_TWO ** ADAM_STEP)
    emb_rows = outs[0].shape[0]

    def update(group, grad_ref, states, source, start, rows, decay_rate):
        width = grad_ref.shape[1]
        cols = ADAM_COLS if width % ADAM_COLS == 0 else width
        at, here = pl.ds(start, rows), pl.ds(source + start, rows)
        for left in range(0, width, cols):
            cs = pl.ds(left, cols)
            grad = grad_ref[here, cs] * clip
            param, mom, var = (ref[here, cs] for ref in states)
            new_mom = BETA_ONE * mom + (1.0 - BETA_ONE) * grad
            new_var = BETA_TWO * var + (1.0 - BETA_TWO) * grad * grad
            move = rate * new_mom / (jnp.sqrt(new_var * bias_two) + ADAM_EPS)
            new_param = (1.0 - LEARN_RATE * decay_rate) * param - move
            for ref, value in zip(news[4 * group:4 * group + 4], (new_param, new_mom, new_var, new_param)):
                ref[at, cs] = value.astype(ref.dtype)
        for k in range(4 * group, 4 * group + 4):
            pltpu.make_async_copy(news[k].at[at], outs[k].at[at], sems.at[k]).start()

    update(2, norm_ref, ins[3:], 0, 0, norm_ref.shape[0], 0.0)
    update(1, mean_ref, ins[:3], emb_rows, 0, outs[4].shape[0], WEIGHT_DECAY)

    def some_rows(r, carry):
        update(0, mean_ref, ins[:3], 0, pl.multiple_of(r * ADAM_ROWS, ADAM_ROWS), ADAM_ROWS, WEIGHT_DECAY)
        return carry

    lax.fori_loop(0, emb_rows // ADAM_ROWS, some_rows, 0)
    for k in range(12):
        pltpu.make_async_copy(outs[k], outs[k], sems.at[k]).wait()


def solution(mesh):
    dev_count = mesh.shape["dp"] * mesh.shape["fsdp"]

    def local_step(emb_grad, mat_grad, norm_grad, emb_param, emb_mom, emb_var, mat_param, mat_mom, mat_var, norm_param, norm_mom, norm_var):
        width = emb_grad.shape[3]
        emb_rows, mat_rows = emb_param.shape[0], mat_param.shape[0]
        count, shard = norm_param.shape
        emb_in = emb_grad.reshape(2, 2, 2, emb_rows, width)
        mat_in = mat_grad.reshape(2, 2, 2, mat_rows, width)
        norm_in = norm_grad.reshape(count, 1, norm_grad.shape[3])
        rows = emb_rows + mat_rows
        main_rows = rows - 8 * LINE_BLOCKS
        rounds = main_rows // 8 * SPLIT
        half = width // 2
        lines = LINE_BLOCKS * LINE_SPLIT
        quarter = width // LINE_SPLIT // 4
        any_spec = pl.BlockSpec(memory_space=pl.ANY)
        vmem_spec = pl.BlockSpec(memory_space=pltpu.VMEM)
        dma = pltpu.SemaphoreType.DMA
        vmem = lambda *shape: pltpu.VMEM(shape, F32)
        mean, norm_mean, scale, param, mom, var = pl.pallas_call(
            functools.partial(reduce_kernel, 1.0 / dev_count),
            out_shape=(
                vmem(rows, width),
                vmem(count, shard),
                vmem(8, LANES),
            ) + (vmem(rows, width),) * 3,
            in_specs=[any_spec] * 9,
            out_specs=(vmem_spec,) * 6,
            scratch_shapes=[
                vmem(2, 2, rows, width),
                vmem(SLOTS, 2, 2, 2, 8, half // SPLIT),
                vmem(2, 2, main_rows, half),
                vmem(2, main_rows, half),
                vmem(main_rows, width),
                vmem(SLOTS, 2, 2, 8, 4 * quarter),
                vmem(lines, 2, 2, 8, 3 * quarter),
                vmem(lines, 2, 2, 8, 2 * quarter),
                vmem(lines, 2, 2, 8, quarter),
                vmem(lines, 2, 8, quarter),
                vmem(lines, 8, quarter),
                vmem(*norm_in.shape),
                vmem(2, 2, count, 1, shard),
                vmem(2, 2, count, 1, shard),
                vmem(2, 2, count, 1, shard),
                vmem(2, count, 1, shard),
                vmem(count, 1, shard),
                vmem(count, 1, shard),
                vmem(count, 1, shard),
                vmem(8, LANES),
                vmem(8, LANES),
                vmem(9, 8, LANES),
                dma, dma((CORE_RING,)), dma((SLOTS,)),
                dma((2,)), dma((2, RING)), dma((2,)), dma((2, RING)),
                dma, dma((2, RING)), dma, dma((2, RING)), dma,
                dma((SLOTS,)), dma((9,)), dma((9, LINE_RING)),
                dma, dma((6,)), dma((6,)), dma, dma, dma, dma, dma((3,)),
            ],
            compiler_params=pltpu.CompilerParams(collective_id=0, has_side_effects=True, vmem_limit_bytes=VMEM_KIB << 10),
            name="reduce_gradients",
        )(*(pltpu.with_memory_space_constraint(a, pltpu.HBM) for a in (
            emb_in, mat_in, norm_in, emb_param, emb_mom, emb_var, mat_param, mat_mom, mat_var)))
        shapes = []
        for like in (emb_param, mat_param, norm_param):
            shapes += [jax.ShapeDtypeStruct(like.shape, F32)] * 3 + [jax.ShapeDtypeStruct(like.shape, jnp.bfloat16)]
        return pl.pallas_call(
            adam_kernel,
            out_shape=tuple(shapes),
            in_specs=[vmem_spec] * 9,
            out_specs=(any_spec,) * 12,
            scratch_shapes=[pltpu.VMEM(like.shape, like.dtype) for like in shapes] + [dma((12,))],
            compiler_params=pltpu.CompilerParams(vmem_limit_bytes=ADAM_MIB << 20),
            name="adam",
        )(scale, mean, norm_mean, param, mom, var, norm_param, norm_mom, norm_var)

    grad_spec = P("dp", "fsdp", None, None)
    row_spec = P("fsdp", None)
    col_spec = P(None, "fsdp")
    in_list = (grad_spec, grad_spec, grad_spec, row_spec, row_spec, row_spec, row_spec, row_spec, row_spec, col_spec, col_spec, col_spec)
    out_list = (row_spec, row_spec, row_spec, row_spec, row_spec, row_spec, row_spec, row_spec, col_spec, col_spec, col_spec, col_spec)
    return jax.shard_map(local_step, mesh=mesh, in_specs=in_list, out_specs=out_list, check_vma=False)
```
